256 devices in a mesh: seq: 8 (over z), exp: 8 (over x, core), tp: 4 (over y).
Axes of the slice: x: 4, y: 4, z: 8, core: 2. Of those that a mesh axis runs over, the one named last changes fastest.
Arguments:
- query_heads: bfloat16 [8192, 32, 128], P(('seq', 'exp'), 'tp'), may hold values from -10 to 10
- key_heads: bfloat16 [8192, 8, 128], P(('seq', 'exp'), 'tp'), may hold values from -10 to 10
- value_head_rows: bfloat16 [8192, 8, 128], P(('seq', 'exp'), 'tp'), may hold values from -6 to 6
- state_input: bfloat16 [8192, 4096], P(('seq', 'exp'), 'tp'), may hold values from -6 to 6
- state_gate: bfloat16 [8192, 4096], P(('seq', 'exp'), 'tp'), may hold values from -6 to 6
- state_inflow: bfloat16 [8192, 8, 128], P(('seq', 'exp'), 'tp'), may hold values from -6 to 6
- state_readout: bfloat16 [8192, 8, 128], P(('seq', 'exp'), 'tp'), may hold values from -6 to 6
- step_size: float32 [8192, 64], P(('seq', 'exp'), 'tp'), may hold values from 0.01 to 0.1
- log_decay: float32 [8192, 64], P(('seq', 'exp'), 'tp'), may hold values from -1 to 0
- skip_scale: float32 [64], P('tp'), may hold values from 0.5 to 2
- state_gain: float32 [4096], P('tp'), may hold values from 0.25 to 1.75
- hidden_in: bfloat16 [8192, 2048], P(('seq', 'exp')), may hold values from -400 to 400
- mlp_gain: float32 [2048], replicated, may hold values from 0.25 to 1.75
- router_weight: bfloat16 [2048, 8], replicated, may hold values from -0.125 to 0.125
- expert_ids: int32 [8192, 2], P(('seq', 'exp')), may hold values from 0 to 7, as said below
- slot_index: int32 [8192, 2], P(('seq', 'exp')), may hold values from -1 to 39, as said below
- gate_up: bfloat16 [8, 7168, 2, 2048], P('exp', ('seq', 'tp')), may hold values from -0.125 to 0.125
- down_proj: bfloat16 [8, 7168, 2048], P('exp', ('seq', 'tp')), may hold values from -0.0625 to 0.0625
Outputs:
- window_out: bfloat16 [8192, 32, 128], P(('seq', 'exp'), 'tp')
- state_out: bfloat16 [8192, 4096], P(('seq', 'exp'), 'tp')
- routed_out: bfloat16 [8192, 2048], P(('seq', 'exp'), 'tp')
The draws below stay inside these ranges and needn't reach their ends.
Inputs may be any that keep to these rules, and one draw needn't show every extreme that they name: `expert_ids`: the 2 ids of a row differ. slot_index[t, k] is the place of the choice expert_ids[t, k] in that expert's buffer of 40 places for the 128 rows of the device block that holds row t (rows b * 128 to b * 128 + 127); the live places of one expert within one block are distinct; -1 marks a dropped choice.
All inputs are finite; a program needn't handle non-finite values.
Results may differ from the reference program's by a relative error of at most 0.02.
Values may be sent and summed in bfloat16 or wider, within the bound.
A program may use at most 128 MiB of HBM per device.

```python
import math
import jax
import jax.numpy as jnp
import numpy as np
from jax import lax

D = 2048
FF = 7168
EXPERTS = 8
TOP = 2
QUERY_HEAD_COUNT = 32
KEY_VALUE_HEADS = 8
HEAD_SIZE = 128
WINDOW = 4096
STATE_HEAD_COUNT = 64
HP = 64
NS = 128
NG = 8
STRETCH = 128
TOK = 128
PROMPT_TOKENS = 8192
CAP = 40


def attention_law(key):
    folded = jax.random.fold_in(key, 101)
    random_subkeys = jax.random.split(folded, 2)
    query_rows = jnp.clip(jax.random.normal(random_subkeys[0], (PROMPT_TOKENS, QUERY_HEAD_COUNT, HEAD_SIZE), jnp.float32), -4.0, 4.0)
    key_row_list = jnp.clip(jax.random.normal(random_subkeys[1], (PROMPT_TOKENS, KEY_VALUE_HEADS, HEAD_SIZE), jnp.float32), -4.0, 4.0)
    return (query_rows, key_row_list)


def draw_query_heads(key, part):
    return attention_law(key)[0].astype(jnp.bfloat16)


def draw_key_heads(key, part):
    return attention_law(key)[1].astype(jnp.bfloat16)


def draw_log_decay(key, part):
    folded = jax.random.fold_in(key, 202)
    random_subkeys = jax.random.split(folded, 7)
    slow_share = 0.5
    gradual_heads = jax.random.uniform(random_subkeys[0], (STATE_HEAD_COUNT,)) < slow_share
    fast_rate = jnp.exp(jax.random.uniform(random_subkeys[1], (STATE_HEAD_COUNT,), minval=math.log(1.0 / 50.0), maxval=math.log(1.0 / 30.0)))
    slow_rate = 0.5 / PROMPT_TOKENS * jnp.exp(jax.random.uniform(random_subkeys[2], (STATE_HEAD_COUNT,), minval=math.log(0.7), maxval=math.log(1.4)))
    head_rate = jnp.where(gradual_heads, slow_rate, fast_rate)
    block_factor = jnp.exp(jax.random.uniform(random_subkeys[3], (PROMPT_TOKENS // TOK, STATE_HEAD_COUNT), minval=math.log(0.6), maxval=math.log(1.5)))
    position_factor = jnp.exp(jax.random.uniform(random_subkeys[4], (PROMPT_TOKENS, STATE_HEAD_COUNT), minval=math.log(0.6), maxval=math.log(1.4)))
    decay_rates = head_rate[None, :] * jnp.repeat(block_factor, TOK, axis=0) * position_factor
    span_rows = jax.random.randint(random_subkeys[5], (3,), 0, PROMPT_TOKENS)
    span_depth = jax.random.uniform(random_subkeys[6], (3, STATE_HEAD_COUNT), minval=0.22, maxval=0.45)
    decay_rates = decay_rates.at[span_rows].add(jnp.where(gradual_heads[None, :], span_depth, 0.0))
    return -decay_rates


def draw_hidden_in(key, part):
    folded = jax.random.fold_in(key, 303)
    random_subkeys = jax.random.split(folded, 3)
    row_scale = jnp.exp(jax.random.uniform(random_subkeys[0], (PROMPT_TOKENS, 1), minval=0.0, maxval=math.log(10.0)))
    column_scale = jnp.exp(jax.random.uniform(random_subkeys[1], (1, D), minval=0.0, maxval=math.log(10.0)))
    values = jnp.clip(jax.random.normal(random_subkeys[2], (PROMPT_TOKENS, D), jnp.float32), -4.0, 4.0)
    return (values * row_scale * column_scale).astype(jnp.bfloat16)


def route_law(key):
    folded = jax.random.fold_in(key, 404)
    random_subkeys = jax.random.split(folded, 5)
    blocks = PROMPT_TOKENS // TOK
    weight_table = np.array([max(1, 4 * EXPERTS // (counter + 1) ** 2) for counter in range(EXPERTS)], np.int32)
    bounds = np.cumsum(weight_table)
    expert_order = jax.random.permutation(random_subkeys[0], EXPERTS)
    ticket = jax.random.randint(random_subkeys[1], (PROMPT_TOKENS,), 0, int(bounds[-1]))
    ranked = jnp.sum(ticket[:, None] >= jnp.asarray(bounds, jnp.int32)[None, :], axis=1)
    block_keys = jax.random.split(random_subkeys[2], blocks)
    forced = jax.vmap(lambda sub: jax.random.permutation(sub, TOK))(block_keys).reshape(PROMPT_TOKENS) < CAP
    ranked = jnp.where(forced, 0, ranked)
    first_pick = expert_order[ranked]
    offset = jax.random.randint(random_subkeys[3], (PROMPT_TOKENS,), 1, EXPERTS)
    second = (first_pick + offset) % EXPERTS
    chosen = jnp.stack([first_pick, second], axis=1).astype(jnp.int32)
    order_keys = jax.random.split(random_subkeys[4], blocks)
    priority = jax.vmap(lambda sub: jax.random.permutation(sub, TOK * TOP))(order_keys)
    flat_ids = chosen.reshape(blocks, TOK * TOP)
    matching = flat_ids[:, :, None] == flat_ids[:, None, :]
    earlier = priority[:, None, :] < priority[:, :, None]
    places = jnp.sum(matching & earlier, axis=-1)
    slot_values = jnp.where(places < CAP, places, -1).reshape(PROMPT_TOKENS, TOP)
    return (chosen, slot_values.astype(jnp.int32))


def draw_expert_ids(key, part):
    return route_law(key)[0]


def draw_slot_index(key, part):
    return route_law(key)[1]


def levels(key, dims, shards, smallest, top_value):
    level, own = 1.0, jax.random.fold_in(key, 6)
    for axis_at, parts in shards:
        draws = jnp.exp(jax.random.uniform(jax.random.fold_in(own, axis_at), (parts,), jnp.float32, smallest / len(shards), top_value / len(shards)))
        level = level * jnp.repeat(draws, dims[axis_at] // parts).reshape([-1 if axis == axis_at else 1 for axis in range(len(dims))])
    return level


def gaussian(own_key, extent, width, most, cuts=(), held_as=jnp.bfloat16):
    gain = levels(own_key, extent, cuts, -0.22, 0.18) if cuts else 1.0
    entries = jax.random.normal(own_key, extent, jnp.float32) * width * gain
    return jnp.minimum(jnp.maximum(entries, -most), most).astype(held_as)


def setup_inputs(seed: int = 0) -> dict:
    keys = jax.random.split(jax.random.key(seed), 19)
    query_heads = draw_query_heads(jax.random.fold_in(keys[18], 71), 0)
    key_heads = draw_key_heads(jax.random.fold_in(keys[18], 71), 0)
    value_head_rows = gaussian(keys[2], (PROMPT_TOKENS, KEY_VALUE_HEADS, HEAD_SIZE), 1.0, 6.0, ((0, 64), (1, 4)))
    state_input = gaussian(keys[3], (PROMPT_TOKENS, STATE_HEAD_COUNT * HP), 1.0, 6.0, ((0, 64), (1, 4)))
    state_gate = gaussian(keys[4], (PROMPT_TOKENS, STATE_HEAD_COUNT * HP), 1.0, 6.0, ((0, 64), (1, 4)))
    state_inflow = gaussian(keys[5], (PROMPT_TOKENS, NG, NS), 1.0, 6.0, ((0, 64), (1, 4)))
    state_readout = gaussian(keys[6], (PROMPT_TOKENS, NG, NS), 1.0, 6.0, ((0, 64), (1, 4)))
    step_size = jnp.clip(jnp.exp(math.log(0.1) - 2.3025851 * jax.random.uniform(keys[7], (PROMPT_TOKENS, STATE_HEAD_COUNT), jnp.float32) ** levels(keys[7], (PROMPT_TOKENS, STATE_HEAD_COUNT), ((0, 64), (1, 4)), -0.2, 0.2)), 0.01, 0.1)
    log_decay = draw_log_decay(jax.random.fold_in(keys[18], 71), 0)
    skip_scale = jnp.clip(jnp.exp(math.log(2.0) - 1.3862944 * jax.random.uniform(keys[9], (STATE_HEAD_COUNT,), jnp.float32) ** levels(keys[9], (STATE_HEAD_COUNT,), ((0, 4),), -0.2, 0.2)), 0.5, 2.0)
    state_gain = jnp.clip(1.0 + 0.15 * jax.random.normal(keys[10], (STATE_HEAD_COUNT * HP,), jnp.float32), 0.25, 1.75)
    hidden_in = draw_hidden_in(jax.random.fold_in(keys[18], 71), 0)
    mlp_gain = jnp.clip(1.0 + 0.15 * jax.random.normal(keys[12], (D,), jnp.float32), 0.25, 1.75)
    router_weight = gaussian(keys[13], (D, EXPERTS), D ** -0.5, 0.125)
    expert_ids = draw_expert_ids(jax.random.fold_in(keys[18], 71), 0)
    slot_index = draw_slot_index(jax.random.fold_in(keys[18], 71), 0)
    gate_up = gaussian(keys[16], (EXPERTS, FF, 2, D), D ** -0.5, 0.125, ((0, 8), (1, 32)))
    down_proj = gaussian(keys[17], (EXPERTS, FF, D), FF ** -0.5, 0.0625, ((0, 8), (1, 32)))
    return dict(query_heads=query_heads, key_heads=key_heads, value_head_rows=value_head_rows, state_input=state_input, state_gate=state_gate, state_inflow=state_inflow, state_readout=state_readout, step_size=step_size, log_decay=log_decay, skip_scale=skip_scale, state_gain=state_gain, hidden_in=hidden_in, mlp_gain=mlp_gain, router_weight=router_weight, expert_ids=expert_ids, slot_index=slot_index, gate_up=gate_up, down_proj=down_proj)


EPSILON = 1e-05

def window_attention(query_heads, key_heads, value_head_rows):
    group_width = QUERY_HEAD_COUNT // KEY_VALUE_HEADS
    query_tile_block = min(PROMPT_TOKENS, 256)
    key_span = WINDOW + query_tile_block
    score_scale = 1.0 / math.sqrt(HEAD_SIZE)
    padded_keys = jnp.pad(key_heads, ((WINDOW, 0), (0, 0), (0, 0)))
    padded_values = jnp.pad(value_head_rows, ((WINDOW, 0), (0, 0), (0, 0)))

    def one_block(counter):
        first_row = counter * query_tile_block
        query_rows = lax.dynamic_slice_in_dim(query_heads, first_row, query_tile_block, 0).astype(jnp.float32)
        query_rows = query_rows.reshape(query_tile_block, KEY_VALUE_HEADS, group_width, HEAD_SIZE)
        key_row_list = lax.dynamic_slice_in_dim(padded_keys, first_row, key_span, 0).astype(jnp.float32)
        value_rows = lax.dynamic_slice_in_dim(padded_values, first_row, key_span, 0).astype(jnp.float32)
        scores = jnp.einsum('qkgd,jkd->kgqj', query_rows, key_row_list, precision=lax.Precision.HIGHEST) * score_scale
        query_pos = first_row + jnp.arange(query_tile_block, dtype=jnp.int32)
        key_pos = first_row - WINDOW + jnp.arange(key_span, dtype=jnp.int32)
        visible = (key_pos[None, :] <= query_pos[:, None]) & (key_pos[None, :] > query_pos[:, None] - WINDOW) & (key_pos[None, :] >= 0)
        scores = jnp.where(visible, scores, -jnp.inf)
        top_score = lax.optimization_barrier(jnp.max(scores, axis=-1, keepdims=True))
        weights = jnp.exp(scores - top_score)
        totals = lax.optimization_barrier(jnp.sum(weights, axis=-1))
        rounded = lax.optimization_barrier(weights.astype(jnp.bfloat16)).astype(jnp.float32)
        outputs = jnp.einsum('kgqj,jkd->qkgd', rounded, value_rows, precision=lax.Precision.HIGHEST)
        outputs = outputs / jnp.transpose(totals, (2, 0, 1))[..., None]
        return outputs.reshape(query_tile_block, QUERY_HEAD_COUNT, HEAD_SIZE).astype(jnp.bfloat16)
    outputs = lax.map(one_block, jnp.arange(PROMPT_TOKENS // query_tile_block, dtype=jnp.int32))
    return outputs.reshape(PROMPT_TOKENS, QUERY_HEAD_COUNT, HEAD_SIZE)

def state_space(state_input, state_gate, state_inflow, state_readout, step_size, log_decay, skip_scale, state_gain):
    stretch_count = PROMPT_TOKENS // STRETCH
    per_group = STATE_HEAD_COUNT // NG
    inputs = state_input.reshape(stretch_count, STRETCH, NG, per_group, HP)
    inflow = state_inflow.reshape(stretch_count, STRETCH, NG, NS)
    readout = state_readout.reshape(stretch_count, STRETCH, NG, NS)
    step_rows = step_size.reshape(stretch_count, STRETCH, NG, per_group)
    decay_rows = log_decay.reshape(stretch_count, STRETCH, NG, per_group)
    causal = (jnp.arange(STRETCH)[:, None] >= jnp.arange(STRETCH)[None, :])[:, :, None, None]

    def advance(carried, packed):
        stretch_in, stretch_inflow, stretch_readout, stretch_steps, stretch_decay = packed
        cumulative = jnp.cumsum(stretch_decay, axis=0)
        read_write = jnp.einsum('ign,jgn->ijg', stretch_readout.astype(jnp.float32), stretch_inflow.astype(jnp.float32), precision=lax.Precision.HIGHEST)
        decay_gap = cumulative[:, None] - cumulative[None, :]
        decay_mat = jnp.where(causal, jnp.exp(jnp.where(causal, decay_gap, 0.0)), 0.0)
        mixing = decay_mat * read_write[..., None] * stretch_steps[None]
        mixing = lax.optimization_barrier(mixing.astype(jnp.bfloat16)).astype(jnp.float32)
        inputs_wide = stretch_in.astype(jnp.float32)
        intra = jnp.einsum('ijgk,jgkp->igkp', mixing, inputs_wide, precision=lax.Precision.HIGHEST)
        stretch_total = cumulative[-1]
        weight_in = jnp.exp(stretch_total[None] - cumulative) * stretch_steps
        weighted = weight_in[..., None] * stretch_inflow.astype(jnp.float32)[:, :, None, :]
        weighted = lax.optimization_barrier(weighted.astype(jnp.bfloat16)).astype(jnp.float32)
        stretch_state = jnp.einsum('jgkn,jgkp->gknp', weighted, inputs_wide, precision=lax.Precision.HIGHEST)
        inter = jnp.exp(cumulative)[..., None] * jnp.einsum('ign,gknp->igkp', stretch_readout.astype(jnp.float32), carried, precision=lax.Precision.HIGHEST)
        carried = jnp.exp(stretch_total)[..., None, None] * carried + stretch_state
        return (carried, intra + inter)
    initial = jnp.zeros((NG, per_group, NS, HP), jnp.float32)
    _, mixed = lax.scan(advance, initial, (inputs, inflow, readout, step_rows, decay_rows))
    skip_rows = skip_scale.reshape(NG, per_group)
    output = mixed + skip_rows[:, :, None] * inputs.astype(jnp.float32)
    gate_rows = state_gate.reshape(stretch_count, STRETCH, NG, per_group, HP).astype(jnp.float32)
    gated = output * jax.nn.silu(gate_rows)
    mean_square = lax.optimization_barrier(jnp.mean(gated * gated, axis=(3, 4), keepdims=True))
    normed = gated * lax.rsqrt(mean_square + EPSILON)
    return (normed.reshape(PROMPT_TOKENS, STATE_HEAD_COUNT * HP) * state_gain).astype(jnp.bfloat16)

def routed_mlp(hidden_in, mlp_gain, router_weight, expert_ids, slot_index, gate_up, down_proj):
    hidden = hidden_in.astype(jnp.float32)
    mean_square = lax.optimization_barrier(jnp.mean(hidden * hidden, axis=-1, keepdims=True))
    normed = (hidden * lax.rsqrt(mean_square + EPSILON) * mlp_gain).astype(jnp.bfloat16)
    logits = jnp.dot(normed, router_weight, preferred_element_type=jnp.float32)
    gate_values = jax.nn.sigmoid(logits)
    chosen = jnp.take_along_axis(gate_values, expert_ids, axis=1)
    mixing = chosen / lax.optimization_barrier(jnp.sum(chosen, axis=1, keepdims=True))
    block_count = PROMPT_TOKENS // TOK
    row_block = jnp.arange(PROMPT_TOKENS, dtype=jnp.int32) // TOK
    is_live = slot_index >= 0
    places = EXPERTS * block_count * CAP
    target = jnp.where(is_live, (expert_ids * block_count + row_block[:, None]) * CAP + slot_index, places)
    buffer = jnp.zeros((places + 1, D), jnp.bfloat16)
    buffer = buffer.at[target.reshape(-1)].set(jnp.repeat(normed, TOP, axis=0))
    expert_inputs = buffer[:-1].reshape(EXPERTS, block_count * CAP, D)

    def one_expert(packed):
        expert_rows, expert_gate_up, expert_down = packed
        rows_wide = expert_rows.astype(jnp.float32)
        gate_part = jnp.dot(rows_wide, expert_gate_up[:, 0, :].astype(jnp.float32).T, precision=lax.Precision.HIGHEST)
        up_part = jnp.dot(rows_wide, expert_gate_up[:, 1, :].astype(jnp.float32).T, precision=lax.Precision.HIGHEST)
        hidden_units = lax.optimization_barrier((jax.nn.silu(gate_part) * up_part).astype(jnp.bfloat16)).astype(jnp.float32)
        return jnp.dot(hidden_units, expert_down.astype(jnp.float32), precision=lax.Precision.HIGHEST)
    outputs = lax.map(one_expert, (expert_inputs, gate_up, down_proj))
    flat_rows = outputs.reshape(places, D)
    picked = flat_rows[jnp.where(is_live, target, 0)]
    weights = jnp.where(is_live, mixing, 0.0)
    return lax.optimization_barrier(jnp.sum(weights[..., None] * picked, axis=1)).astype(jnp.bfloat16)

def reference(query_heads, key_heads, value_head_rows, state_input, state_gate, state_inflow, state_readout, step_size, log_decay, skip_scale, state_gain, hidden_in, mlp_gain, router_weight, expert_ids, slot_index, gate_up, down_proj):
    window_out = window_attention(query_heads, key_heads, value_head_rows)
    state_out = state_space(state_input, state_gate, state_inflow, state_readout, step_size, log_decay, skip_scale, state_gain)
    routed_out = routed_mlp(hidden_in, mlp_gain, router_weight, expert_ids, slot_index, gate_up, down_proj)
    return (window_out, state_out, routed_out)
```

```python
import functools
import math

import jax
import jax.numpy as jnp
from jax import lax
from jax.experimental import pallas as pl
from jax.experimental.pallas import tpu as pltpu
from jax.sharding import PartitionSpec as P

EXPERTS = 8
CAP = 40
STEPS = 8
CORES = 8
TPS = 4
QUARTER = 10
PAD = 16
ROWS = 80
EPSILON = 1e-05
VM = pltpu.VMEM
MESH = pl.DeviceIdType.MESH
F32 = jnp.float32
BF16 = jnp.bfloat16


def rcopy(src, dst, ss, rs, dev):
    return pltpu.make_async_remote_copy(
        src_ref=src, dst_ref=dst, send_sem=ss, recv_sem=rs, device_id=dev, device_id_type=MESH
    )


def guarded(cond, fn):
    if cond is True:
        fn()
    else:
        pl.when(cond)(fn)


def greet(groups):
    barrier = pltpu.get_barrier_semaphore()
    count = 0
    for axis, size, shifts in groups:
        me = lax.axis_index(axis)
        for d in shifts:
            pl.semaphore_signal(
                barrier, inc=1, device_id={axis: lax.rem(me + d, size)}, device_id_type=MESH
            )
            count += 1
    pl.semaphore_wait(barrier, count)


def spread_kernel(
    kv_in, rows_in, pack, st_in, dec_s, dec_o,
    kv, rows, ent,
    disp, st_rx, t_tx, t_rx, ent_tx, inner, carry,
    z_s, z_r, x_s, x_r, p_s, p_r, f_s, f_r,
    d_s, d_r, rf_s, rf_r, rb_s, rb_r, sa_s, sa_r, st_s, st_r, se_s, se_r,
):
    s = lax.axis_index("seq")
    e = lax.axis_index("exp")
    x = e // 2
    c = lax.rem(e, 2)
    partner = e + 1 - 2 * c
    nxt = lax.rem(s + 1, STEPS)
    prv = lax.rem(s + STEPS - 1, STEPS)
    greet((("exp", CORES, range(1, CORES)), ("seq", STEPS, range(1, STEPS))))
    pending = []

    def send(copy, cond=True):
        guarded(cond, copy.start)
        pending.append((copy, cond))

    def slot_of(k):
        return 32 if k == 4 else k * 8 + e

    def block(k):
        return kv_in if k == 0 else kv.at[:, slot_of(k)]

    def kv_hop(k):
        return rcopy(
            block(k - 1), kv.at[:, slot_of(k)], z_s.at[k - 1], z_r.at[k - 1], {"seq": nxt}
        )

    def kv_across(g, k):
        for dx in range(1, 4):
            tx = lax.rem(x + dx, 4)
            if k == 0:
                cond = tx > x
            elif k == 4:
                cond = (tx < x) & (s >= 4)
            else:
                cond = s >= k
            send(
                rcopy(
                    block(k), kv.at[:, g * 8 + e], x_s.at[k, dx], x_r.at[g, dx],
                    {"exp": 2 * tx + c},
                ),
                cond,
            )
        if k == 0:
            cond = c == 0
        elif k == 4:
            cond = (c == 1) & (s >= 4)
        else:
            cond = s >= k
        send(
            rcopy(block(k), kv.at[:, g * 8 + e], p_s.at[k], p_r.at[g], {"exp": partner}), cond
        )

    def kv_forward(g):
        for dx in range(1, 4):
            sx = lax.rem(x + 4 - dx, 4)
            cond = ((sx < x) | (s >= 4)) if g == 0 else s >= g
            slot = kv.at[:, g * 8 + 2 * sx + c]
            arrived = rcopy(slot, slot, x_s.at[g, dx], x_r.at[g, dx], {"exp": 2 * sx + c})
            onward = rcopy(slot, slot, f_s.at[g, dx], f_r.at[g, dx], {"exp": partner})

            def pass_on(arrived=arrived, onward=onward):
                arrived.wait_recv()
                onward.start()

            guarded(cond, pass_on)
            pending.append((onward, cond))

    def kv_finish(g):
        slot = kv.at[:, g * 8 + partner]
        cond = ((c == 1) | (s >= 4)) if g == 0 else s >= g
        guarded(cond, rcopy(slot, slot, p_s.at[g], p_r.at[g], {"exp": partner}).wait_recv)
        for dx in range(1, 4):
            sx = lax.rem(x + 4 - dx, 4)
            cond = ((sx < x) | (s >= 4)) if g == 0 else s >= g
            slot = kv.at[:, g * 8 + 2 * sx + 1 - c]
            guarded(
                cond, rcopy(slot, slot, f_s.at[g, dx], f_r.at[g, dx], {"exp": partner}).wait_recv
            )

    for d in range(1, CORES):
        to = lax.rem(e + d, CORES)
        send(rcopy(rows_in.at[to], disp.at[e], d_s.at[d], d_r.at[d], {"exp": to}))
    send(kv_hop(1), s < STEPS - 1)
    for d in range(1, CORES):
        to = lax.rem(e + d, CORES)
        send(rcopy(st_in.at[to], st_rx.at[e], sa_s.at[d], sa_r.at[d], {"exp": to}))
    kv_across(0, 0)
    kv[:, pl.ds(e, 1)] = kv_in[...][:, None]
    disp[pl.ds(e, 1)] = rows_in[pl.ds(e, 1)]
    st_rx[pl.ds(e, 1)] = st_in[pl.ds(e, 1)]

    for d in range(1, CORES):
        frm = lax.rem(e + CORES - d, CORES)
        rcopy(disp.at[frm], disp.at[frm], d_s.at[d], d_r.at[d], {"exp": frm}).wait_recv()
    packed = jnp.dot(
        pack[...], disp[...].reshape(CORES * PAD, -1), preferred_element_type=F32
    ).astype(BF16)
    rows[pl.ds(s, 1)] = packed[None]

    def rows_up(j):
        at = rows.at[lax.rem(s + STEPS - j, STEPS)]
        return rcopy(at, at, rf_s.at[j], rf_r.at[j], {"seq": nxt})

    def rows_down(j):
        at = rows.at[lax.rem(s + j, STEPS)]
        return rcopy(at, at, rb_s.at[j], rb_r.at[j], {"seq": prv})

    def rows_up_arrived(j):
        at = rows.at[lax.rem(s + STEPS - 1 - j, STEPS)]
        return rcopy(at, at, rf_s.at[j], rf_r.at[j], {"seq": prv})

    def rows_down_arrived(j):
        at = rows.at[lax.rem(s + 1 + j, STEPS)]
        return rcopy(at, at, rb_s.at[j], rb_r.at[j], {"seq": nxt})

    send(rows_up(0))
    send(rows_down(0))

    for d in range(1, CORES):
        frm = lax.rem(e + CORES - d, CORES)
        rcopy(st_rx.at[frm], st_rx.at[frm], sa_s.at[d], sa_r.at[d], {"exp": frm}).wait_recv()
    for h in range(2):
        part = slice(64 * h, 64 * h + 64)
        run = jnp.zeros((64, 128), F32)
        for k in range(CORES):
            inner[k, part, :] = run
            run = run * dec_s[k, h] + st_rx[k, part, :].astype(F32)
        t_tx[part, :] = run.astype(BF16)
    for d in range(1, STEPS):
        to = lax.rem(s + d, STEPS)
        send(rcopy(t_tx, t_rx.at[s], st_s.at[d], st_r.at[d], {"seq": to}), s + d < STEPS)

    def kv_arrive(k):
        slot = kv.at[:, slot_of(k)]
        guarded(
            s >= k, rcopy(slot, slot, z_s.at[k - 1], z_r.at[k - 1], {"seq": prv}).wait_recv
        )
        if k < 4:
            send(kv_hop(k + 1), (s >= k) & (s < STEPS - 1))
        kv_across(0 if k == 4 else k, k)

    for j in range(4):
        kv_arrive(j + 1)
        if j < 3:
            rows_up_arrived(j).wait_recv()
            if j < 2:
                send(rows_up(j + 1))
        if j >= 1:
            kv_forward(j)
        if j == 0:
            for d in range(1, STEPS):
                frm = lax.rem(s + STEPS - d, STEPS)
                at = t_rx.at[frm]
                guarded(
                    d <= s, rcopy(at, at, st_s.at[d], st_r.at[d], {"seq": frm}).wait_recv
                )
            carry[...] = jnp.zeros_like(carry)
            for k in range(STEPS - 1):

                def fold(k=k):
                    for h in range(2):
                        part = slice(64 * h, 64 * h + 64)
                        carry[part, :] = carry[part, :] * dec_o[k, h] + t_rx[
                            k, part, :
                        ].astype(F32)

                pl.when(k < s)(fold)
            for h in range(2):
                part = slice(64 * h, 64 * h + 64)
                moved = carry[part, :]
                for k in range(CORES):
                    ent_tx[k, part, :] = (inner[k, part, :] + moved).astype(BF16)
                    moved = moved * dec_s[k, h]
            for d in range(1, CORES):
                to = lax.rem(e + d, CORES)
                send(rcopy(ent_tx.at[to], ent.at[e], se_s.at[d], se_r.at[d], {"exp": to}))
            ent[pl.ds(e, 1)] = ent_tx[pl.ds(e, 1)]
        rows_down_arrived(j).wait_recv()
        if j < 3:
            send(rows_down(j + 1))
    kv_forward(0)
    for g in (1, 2, 3, 0):
        kv_finish(g)
    for d in range(1, CORES):
        frm = lax.rem(e + CORES - d, CORES)
        rcopy(ent.at[frm], ent.at[frm], se_s.at[d], se_r.at[d], {"exp": frm}).wait_recv()
    for copy, cond in pending:
        guarded(cond, copy.wait_send)


def spread(kv_in, rows_in, pack, st_in, dec_s, dec_o):
    vm = pl.BlockSpec(memory_space=VM)
    sm = pl.BlockSpec(memory_space=pltpu.SMEM)
    width = rows_in.shape[-1]
    dma = pltpu.SemaphoreType.DMA
    return pl.pallas_call(
        spread_kernel,
        out_shape=(
            jax.ShapeDtypeStruct((4, 33, 128, 128), BF16),
            jax.ShapeDtypeStruct((STEPS, ROWS, width), BF16),
            jax.ShapeDtypeStruct((CORES, 128, 128), BF16),
        ),
        in_specs=[vm, vm, vm, vm, sm, sm],
        out_specs=(vm, vm, vm),
        scratch_shapes=[
            VM((CORES, PAD, width), BF16),
            VM((CORES, 128, 128), BF16),
            VM((128, 128), BF16),
            VM((STEPS, 128, 128), BF16),
            VM((CORES, 128, 128), BF16),
            VM((CORES, 128, 128), F32),
            VM((128, 128), F32),
            dma((4,)), dma((4,)), dma((5, 4)), dma((4, 4)), dma((5,)), dma((4,)),
            dma((4, 4)), dma((4, 4)),
            dma((8,)), dma((8,)), dma((3,)), dma((3,)), dma((4,)), dma((4,)),
            dma((8,)), dma((8,)), dma((8,)), dma((8,)), dma((8,)), dma((8,)),
        ],
        compiler_params=pltpu.CompilerParams(
            collective_id=1, has_side_effects=True, vmem_limit_bytes=40 << 20
        ),
        cost_estimate=pl.CostEstimate(
            flops=30_000_000_000, bytes_accessed=20_000_000, transcendentals=0
        ),
        name="spread",
    )(kv_in, rows_in, pack, st_in, dec_s, dec_o)


def attention_kernel(q, kv, out):
    s = lax.axis_index("seq")
    e = lax.axis_index("exp")
    row = lax.broadcasted_iota(jnp.int32, (128, 1024), 0)
    col = lax.broadcasted_iota(jnp.int32, (128, 1024), 1)
    place = col // 128
    inside = lax.rem(col, 128)
    far_ok = s >= 4
    near = (place < e) | ((place == e) & (inside <= row)) | ((place > e) & far_ok)
    vrow = lax.broadcasted_iota(jnp.int32, (1024, 128), 0) // 128
    v_ok = (vrow <= e) | far_ok
    last = (lax.broadcasted_iota(jnp.int32, (128, 128), 1) > lax.broadcasted_iota(
        jnp.int32, (128, 128), 0)) & far_ok
    scale = 1.0 / math.sqrt(128)

    def chunk(carried, query, keys, values, mask):
        top, total, acc = carried
        scores = lax.dot_general(
            query, keys, (((1,), (1,)), ((), ())), preferred_element_type=F32
        ) * scale
        if mask is not None:
            scores = jnp.where(mask, scores, -1e30)
        new = jnp.maximum(top, jnp.max(scores, axis=1, keepdims=True))
        weights = jnp.exp(scores - new)
        if mask is not None:
            weights = jnp.where(mask, weights, 0.0)
        factor = jnp.exp(top - new)
        total = total * factor + jnp.sum(weights, axis=1, keepdims=True)
        acc = acc * factor + jnp.dot(
            weights.astype(BF16), values, preferred_element_type=F32
        )
        return new, total, acc

    def one_head(h, _):
        group = h // 4
        query = q[h]
        k0 = kv[group, 0:8].reshape(1024, 128)
        v0 = jnp.where(v_ok, kv[2 + group, 0:8].reshape(1024, 128), jnp.zeros((), BF16))
        state = (
            jnp.full((128, 1), -1e30, F32),
            jnp.zeros((128, 1), F32),
            jnp.zeros((128, 128), F32),
        )
        state = chunk(state, query, k0, v0, near)
        vl = jnp.where(far_ok, kv[2 + group, 32], jnp.zeros((), BF16))
        state = chunk(state, query, kv[group, 32], vl, last)

        def more(k, carried):
            keys = kv[group, pl.ds(k * 8, 8)].reshape(1024, 128)
            values = kv[2 + group, pl.ds(k * 8, 8)].reshape(1024, 128)
            return chunk(carried, query, keys, values, None)

        _, total, acc = lax.fori_loop(1, jnp.minimum(s, 3) + 1, more, state)
        out[h] = (acc / total).astype(BF16)
        return 0

    lax.fori_loop(0, 8, one_head, 0)


def attention(q, kv):
    vm = pl.BlockSpec(memory_space=VM)
    return pl.pallas_call(
        attention_kernel,
        out_shape=jax.ShapeDtypeStruct((8, 128, 128), BF16),
        in_specs=[vm, vm],
        out_specs=vm,
        compiler_params=pltpu.CompilerParams(vmem_limit_bytes=40 << 20),
        cost_estimate=pl.CostEstimate(
            flops=10_000_000_000, bytes_accessed=5_000_000, transcendentals=4_000_000
        ),
        name="attend",
    )(q, kv)


def summary_kernel(inputs, inflow, weight_in, out):
    for pair in range(8):
        vectors = inflow[:, 128 * (pair // 4):128 * (pair // 4) + 128].astype(F32)
        both = inputs[:, 128 * pair:128 * pair + 128]
        for h in range(2):
            head = 2 * pair + h
            weighted = (weight_in[:, head:head + 1] * vectors).astype(BF16)
            res = lax.dot_general(
                both, weighted, (((0,), (0,)), ((), ())), preferred_element_type=F32
            )
            out[pair, 64 * h:64 * h + 64, :] = res[64 * h:64 * h + 64].astype(BF16)


def summary(inputs, inflow, weight_in):
    vm = pl.BlockSpec(memory_space=VM)
    return pl.pallas_call(
        summary_kernel,
        out_shape=jax.ShapeDtypeStruct((8, 128, 128), BF16),
        in_specs=[vm] * 3,
        out_specs=vm,
        cost_estimate=pl.CostEstimate(
            flops=1_000_000_000, bytes_accessed=1_000_000, transcendentals=0
        ),
        name="summary",
    )(inputs, inflow, weight_in)


def state_kernel(inputs, gate, inflow, readout, cum, cum_t, step_t, skip, gain, ent, out, gated):
    low = lax.broadcasted_iota(jnp.int32, (128, 128), 1) < 64
    causal = lax.broadcasted_iota(jnp.int32, (128, 128), 0) >= lax.broadcasted_iota(
        jnp.int32, (128, 128), 1)
    for g in range(2):
        cols = slice(128 * g, 128 * g + 128)
        read = readout[:, cols]
        rw = lax.dot_general(
            read, inflow[:, cols], (((1,), (1,)), ((), ())), preferred_element_type=F32
        )
        square = jnp.zeros((128, 1), F32)
        for p in range(4):
            pair = 4 * g + p
            at = slice(128 * pair, 128 * pair + 128)
            both = inputs[:, at]
            parts = []
            scales = []
            for h in range(2):
                head = 2 * pair + h
                own = cum[:, head:head + 1]
                gap = jnp.where(causal, own - cum_t[head:head + 1, :], 0.0)
                mixing = jnp.where(causal, jnp.exp(gap), 0.0) * rw * step_t[head:head + 1, :]
                parts.append(
                    jnp.dot(mixing.astype(BF16), both, preferred_element_type=F32)
                )
                scales.append(jnp.exp(own))
            intra = jnp.where(low, parts[0], parts[1])
            scale = jnp.where(low, scales[0], scales[1])
            inter = scale * lax.dot_general(
                read, ent[pair], (((1,), (1,)), ((), ())), preferred_element_type=F32
            )
            mixed = intra + inter + skip[:, at] * both.astype(F32)
            v = gate[:, at].astype(F32)
            value = mixed * (v / (1.0 + jnp.exp(-v)))
            gated[:, 128 * p:128 * p + 128] = value
            square = square + jnp.sum(value * value, axis=1, keepdims=True)
        inv = lax.rsqrt(square / 512.0 + EPSILON)
        wide = slice(512 * g, 512 * g + 512)
        out[:, wide] = (gated[...] * inv * gain[:, wide]).astype(BF16)


def state_out_of(inputs, gate, inflow, readout, cum, cum_t, step_t, skip, gain, ent):
    vm = pl.BlockSpec(memory_space=VM)
    return pl.pallas_call(
        state_kernel,
        out_shape=jax.ShapeDtypeStruct((128, 1024), BF16),
        in_specs=[vm] * 10,
        out_specs=vm,
        scratch_shapes=[VM((128, 512), F32)],
        cost_estimate=pl.CostEstimate(
            flops=4_000_000_000, bytes_accessed=2_000_000, transcendentals=400_000
        ),
        name="state",
    )(inputs, gate, inflow, readout, cum, cum_t, step_t, skip, gain, ent)


def gather_kernel(
    part, unpack, weigh, out,
    tx, rx, slots_tx, slots, mine_tx, mine,
    r_s, r_r, x_s, x_r, y_s, y_r,
):
    s = lax.axis_index("seq")
    e = lax.axis_index("exp")
    t = lax.axis_index("tp")
    nxt = lax.rem(s + 1, STEPS)
    prv = lax.rem(s + STEPS - 1, STEPS)
    greet(
        (
            ("exp", CORES, range(1, CORES)),
            ("seq", STEPS, (1, STEPS - 1)),
            ("tp", TPS, range(1, TPS)),
        )
    )
    pending = []
    width = part.shape[-1] // 4

    def columns(stream):
        return slice(width * stream, width * stream + width)

    def ring(stream, j):
        to = nxt if stream < 2 else prv
        return rcopy(
            tx.at[stream, j], rx.at[stream, j], r_s.at[stream, j], r_r.at[stream, j], {"seq": to}
        )

    def owner(stream, j):
        if stream < 2:
            return lax.rem(s + 2 * STEPS - 1 - j, STEPS)
        return lax.rem(s + 1 + j, STEPS)

    order = (0, 2, 1, 3)
    for j in range(STEPS - 1):
        for stream in order:
            q = owner(stream, j)
            value = part[q, :, columns(stream)]
            if j > 0:
                ring(stream, j - 1).wait_recv()
                value = (value.astype(F32) + rx[stream, j - 1].astype(F32)).astype(BF16)
            tx[stream, j] = value
            copy = ring(stream, j)
            copy.start()
            pending.append(copy)
    for stream in order:
        ring(stream, STEPS - 2).wait_recv()
        total = part[s, :, columns(stream)].astype(F32) + rx[stream, STEPS - 2].astype(F32)
        spaced = jnp.dot(unpack[...], total.astype(BF16), preferred_element_type=F32)
        slots_tx[:, :, columns(stream)] = spaced.astype(BF16).reshape(CORES, PAD, width)
    for d in range(1, CORES):
        to = lax.rem(e + d, CORES)
        copy = rcopy(slots_tx.at[to], slots.at[e], x_s.at[d], x_r.at[d], {"exp": to})
        copy.start()
        pending.append(copy)
    slots[pl.ds(e, 1)] = slots_tx[pl.ds(e, 1)]
    for d in range(1, CORES):
        frm = lax.rem(e + CORES - d, CORES)
        at = slots.at[frm]
        rcopy(at, at, x_s.at[d], x_r.at[d], {"exp": frm}).wait_recv()
    high = weigh[...].astype(BF16)
    rest = (weigh[...] - high.astype(F32)).astype(BF16)
    for quarter in range(TPS):
        at = slots[:, :, columns(quarter)].reshape(CORES * PAD, width)
        mine_tx[quarter] = (
            jnp.dot(high, at, preferred_element_type=F32)
            + jnp.dot(rest, at, preferred_element_type=F32)
        ).astype(BF16)
    for d in range(1, TPS):
        to = lax.rem(t + d, TPS)
        copy = rcopy(mine_tx.at[to], mine.at[d], y_s.at[d], y_r.at[d], {"tp": to})
        copy.start()
        pending.append(copy)
    total = mine_tx[t].astype(F32)
    for d in range(1, TPS):
        frm = lax.rem(t + TPS - d, TPS)
        at = mine.at[d]
        rcopy(at, at, y_s.at[d], y_r.at[d], {"tp": frm}).wait_recv()
        total = total + mine[d].astype(F32)
    out[...] = total.astype(BF16)
    for copy in pending:
        copy.wait_send()


def gathered(part, unpack, weigh):
    vm = pl.BlockSpec(memory_space=VM)
    width = part.shape[-1]
    q = width // 4
    dma = pltpu.SemaphoreType.DMA
    return pl.pallas_call(
        gather_kernel,
        out_shape=jax.ShapeDtypeStruct((128, q), BF16),
        in_specs=[vm] * 3,
        out_specs=vm,
        scratch_shapes=[
            VM((4, STEPS - 1, ROWS, q), BF16),
            VM((4, STEPS - 1, ROWS, q), BF16),
            VM((CORES, PAD, width), BF16),
            VM((CORES, PAD, width), BF16),
            VM((TPS, 128, q), BF16),
            VM((TPS, 128, q), BF16),
            dma((4, STEPS - 1)), dma((4, STEPS - 1)), dma((8,)), dma((8,)), dma((4,)), dma((4,)),
        ],
        compiler_params=pltpu.CompilerParams(
            collective_id=2, has_side_effects=True, vmem_limit_bytes=40 << 20
        ),
        name="collect",
    )(part, unpack, weigh)


def local(
    query_heads, key_heads, value_head_rows, state_input, state_gate, state_inflow,
    state_readout, step_size, log_decay, skip_scale, state_gain, hidden_in, mlp_gain,
    router_weight, expert_ids, slot_index, gate_up, down_proj,
):
    s = lax.axis_index("seq")
    e = lax.axis_index("exp")
    tp = lax.axis_index("tp")
    wide_gate_up = lax.all_gather(gate_up, "tp", axis=1, tiled=True)
    wide_down = lax.all_gather(down_proj, "tp", axis=1, tiled=True)

    hidden = hidden_in.astype(F32)
    mean_square = jnp.mean(hidden * hidden, axis=-1, keepdims=True)
    normed = (hidden * lax.rsqrt(mean_square + EPSILON) * mlp_gain).astype(BF16)
    gate_values = jax.nn.sigmoid(jnp.dot(normed, router_weight, preferred_element_type=F32))
    one_hot = expert_ids[..., None] == jnp.arange(EXPERTS, dtype=jnp.int32)
    chosen = jnp.sum(jnp.where(one_hot, gate_values[:, None, :], 0.0), axis=-1)
    mixing = chosen / jnp.sum(chosen, axis=1, keepdims=True)
    is_live = slot_index >= 0
    inside = slot_index - tp * QUARTER
    taken = is_live & (inside >= 0) & (inside < QUARTER)
    place = jnp.where(taken, expert_ids * PAD + inside, -1)
    hits = place[..., None] == jnp.arange(EXPERTS * PAD, dtype=jnp.int32)
    picker = jnp.any(hits, axis=1).astype(BF16)
    weigh = jnp.sum(jnp.where(hits, mixing[..., None], 0.0), axis=1)
    outgoing = lax.dot_general(
        picker, normed, (((0,), (0,)), ((), ())), preferred_element_type=F32
    ).astype(BF16).reshape(EXPERTS, PAD, -1)
    flat = jnp.arange(ROWS)
    pack = ((flat // QUARTER) * PAD + flat % QUARTER)[:, None] == jnp.arange(CORES * PAD)[None]
    pack = pack.astype(BF16)

    cum = jnp.cumsum(log_decay, axis=0)
    block_total = cum[-1]
    weight_in = jnp.exp(block_total[None] - cum) * step_size
    states = summary(state_input, state_inflow.reshape(128, 256), weight_in)
    totals = lax.all_gather(lax.all_gather(block_total, "exp"), "seq")
    mine = lax.dynamic_slice_in_dim(totals, 2 * e, 2, 2)
    dec_s = jnp.exp(lax.dynamic_index_in_dim(mine, s, 0, keepdims=False))
    dec_o = jnp.exp(jnp.sum(mine, axis=1))

    kv_in = jnp.concatenate(
        [jnp.transpose(key_heads, (1, 0, 2)), jnp.transpose(value_head_rows, (1, 0, 2))], axis=0
    )
    kv, rows, entering = spread(kv_in, outgoing, pack, states, dec_s, dec_o)

    heads = attention(jnp.transpose(query_heads, (1, 0, 2)), kv)
    window_out = jnp.transpose(heads, (1, 0, 2))
    state_out = state_out_of(
        state_input, state_gate, state_inflow.reshape(128, 256), state_readout.reshape(128, 256),
        cum, cum.T, step_size.T, jnp.repeat(skip_scale, 64)[None], state_gain[None], entering,
    )

    flat_rows = rows.reshape(STEPS * ROWS, -1)
    projected = jnp.einsum(
        "rd,fsd->srf", flat_rows, wide_gate_up[0], preferred_element_type=F32
    )
    hidden_units = (jax.nn.silu(projected[0]) * projected[1]).astype(BF16)
    part = jnp.dot(hidden_units, wide_down[0], preferred_element_type=F32).astype(BF16)
    routed_out = gathered(part.reshape(STEPS, ROWS, -1), pack.T, weigh)
    return window_out, state_out, routed_out


def solution(mesh):
    both = ("seq", "exp")
    placed = (
        P(both, "tp", None), P(both, "tp", None), P(both, "tp", None),
        P(both, "tp"), P(both, "tp"), P(both, "tp", None), P(both, "tp", None),
        P(both, "tp"), P(both, "tp"), P("tp"), P("tp"), P(both, None), P(), P(),
        P(both, None), P(both, None),
        P("exp", ("seq", "tp"), None, None), P("exp", ("seq", "tp"), None),
    )
    return jax.shard_map(
        local,
        mesh=mesh,
        in_specs=placed,
        out_specs=(P(both, "tp", None), P(both, "tp"), P(both, "tp")),
        check_vma=False,
    )
```

```python
import functools
import math

import jax
import jax.numpy as jnp
from jax import lax
from jax.experimental import pallas as pl
from jax.experimental.pallas import tpu as pltpu
from jax.sharding import PartitionSpec as P

EXPERTS = 8
CAP = 40
STEPS = 8
CORES = 8
TPS = 4
QUARTER = 10
PAD = 16
ROWS = 80
UNITS = 448
HALF = 112
EPSILON = 1e-05
VM = pltpu.VMEM
MESH = pl.DeviceIdType.MESH
F32 = jnp.float32
BF16 = jnp.bfloat16


def rcopy(src, dst, ss, rs, dev):
    return pltpu.make_async_remote_copy(
        src_ref=src, dst_ref=dst, send_sem=ss, recv_sem=rs, device_id=dev, device_id_type=MESH
    )


def guarded(cond, fn):
    if cond is True:
        fn()
    else:
        pl.when(cond)(fn)


def greet(groups):
    barrier = pltpu.get_barrier_semaphore()
    count = 0
    for axis, size, shifts in groups:
        me = lax.axis_index(axis)
        for d in shifts:
            pl.semaphore_signal(
                barrier, inc=1, device_id={axis: lax.rem(me + d, size)}, device_id_type=MESH
            )
            count += 1
    pl.semaphore_wait(barrier, count)


def attend_body(s, e, q, kv, out):
    row = lax.rem(lax.broadcasted_iota(jnp.int32, (512, 1024), 0), 128)
    col = lax.broadcasted_iota(jnp.int32, (512, 1024), 1)
    place = col // 128
    inside = lax.rem(col, 128)
    far_ok = s >= 4
    near = (place < e) | ((place == e) & (inside <= row)) | ((place > e) & far_ok)
    vrow = lax.broadcasted_iota(jnp.int32, (1024, 128), 0) // 128
    v_ok = (vrow <= e) | far_ok
    last = (
        lax.broadcasted_iota(jnp.int32, (512, 128), 1)
        > lax.rem(lax.broadcasted_iota(jnp.int32, (512, 128), 0), 128)
    ) & far_ok
    scale = 1.0 / math.sqrt(128) * math.log2(math.e)

    def chunk(carried, query, keys, values, mask):
        top, total, acc = carried
        scores = lax.dot_general(
            query, keys, (((1,), (1,)), ((), ())), preferred_element_type=F32
        )
        if mask is not None:
            scores = jnp.where(mask, scores, -1e30)
        new = jnp.maximum(top, jnp.max(scores, axis=1, keepdims=True))
        weights = jnp.exp2((scores - new) * scale)
        if mask is not None:
            weights = jnp.where(mask, weights, 0.0)
        factor = jnp.exp2((top - new) * scale)
        total = total * factor + jnp.sum(weights, axis=1, keepdims=True)
        acc = acc * factor + jnp.dot(
            weights.astype(BF16), values, preferred_element_type=F32
        )
        return new, total, acc

    def one_group(group, _):
        query = q[group]
        k0 = kv[group, 0:8].reshape(1024, 128)
        v0 = jnp.where(v_ok, kv[2 + group, 0:8].reshape(1024, 128), jnp.zeros((), BF16))
        state = (
            jnp.full((512, 1), -1e30, F32),
            jnp.zeros((512, 1), F32),
            jnp.zeros((512, 128), F32),
        )
        state = chunk(state, query, k0, v0, near)
        vl = jnp.where(far_ok, kv[2 + group, 32], jnp.zeros((), BF16))
        state = chunk(state, query, kv[group, 32], vl, last)

        def more(k, carried):
            keys = kv[group, pl.ds(k * 8, 8)].reshape(1024, 128)
            values = kv[2 + group, pl.ds(k * 8, 8)].reshape(1024, 128)
            return chunk(carried, query, keys, values, None)

        _, total, acc = lax.fori_loop(1, jnp.minimum(s, 3) + 1, more, state)
        out[group] = (acc / total).astype(BF16)
        return 0

    lax.fori_loop(0, 2, one_group, 0)


def spread_kernel(
    kv_in, rows_in, pack, st_in, dec_in, gu_in, dn_in, q,
    inputs, gate, inflow, readout, cum, cum_t, step_t, skip, gain,
    heads, state_out, h_all, h_oth, dn,
    gu, kv, rows, ent, disp, st_rx, dec_rx, t_tx, t_rx, td_tx, td_rx, ent_tx, inner, carry, gated,
    l_s, g_s, g_r, n_s, n_r, h_s, h_r,
    z_s, z_r, x_s, x_r, p_s, p_r, f_s, f_r,
    d_s, d_r, rf_s, rf_r, rb_s, rb_r, sa_s, sa_r, da_s, da_r, st_s, st_r, sd_s, sd_r, se_s, se_r,
):
    s = lax.axis_index("seq")
    e = lax.axis_index("exp")
    t = lax.axis_index("tp")
    x = e // 2
    c = lax.rem(e, 2)
    partner = e + 1 - 2 * c
    nxt = lax.rem(s + 1, STEPS)
    prv = lax.rem(s + STEPS - 1, STEPS)
    odd = lax.rem(t, 2)
    to_a = {"tp": t + 1 - 2 * odd}
    to_b = {"tp": lax.rem(t + 3 + 2 * odd, TPS)}
    to_mate = {"tp": lax.rem(t + 2, TPS)}
    greet(
        (
            ("tp", TPS, range(1, TPS)),
            ("exp", CORES, range(1, CORES)),
            ("seq", STEPS, range(1, STEPS)),
        )
    )
    pending = []

    def send(copy, cond=True):
        guarded(cond, copy.start)
        pending.append((copy, cond))

    def slot_of(k):
        return 32 if k == 4 else k * 8 + e

    def block(k):
        return kv_in if k == 0 else kv.at[:, slot_of(k)]

    def kv_hop(k):
        return rcopy(
            block(k - 1), kv.at[:, slot_of(k)], z_s.at[k - 1], z_r.at[k - 1], {"seq": nxt}
        )

    def kv_across(g, k):
        for dx in range(1, 4):
            tx = lax.rem(x + dx, 4)
            if k == 0:
                cond = tx > x
            elif k == 4:
                cond = (tx < x) & (s >= 4)
            else:
                cond = s >= k
            send(
                rcopy(
                    block(k), kv.at[:, g * 8 + e], x_s.at[k, dx], x_r.at[g, dx],
                    {"exp": 2 * tx + c},
                ),
                cond,
            )
        if k == 0:
            cond = c == 0
        elif k == 4:
            cond = (c == 1) & (s >= 4)
        else:
            cond = s >= k
        send(
            rcopy(block(k), kv.at[:, g * 8 + e], p_s.at[k], p_r.at[g], {"exp": partner}), cond
        )

    def kv_forward(g):
        for dx in range(1, 4):
            sx = lax.rem(x + 4 - dx, 4)
            cond = ((sx < x) | (s >= 4)) if g == 0 else s >= g
            slot = kv.at[:, g * 8 + 2 * sx + c]
            arrived = rcopy(slot, slot, x_s.at[g, dx], x_r.at[g, dx], {"exp": 2 * sx + c})
            onward = rcopy(slot, slot, f_s.at[g, dx], f_r.at[g, dx], {"exp": partner})

            def pass_on(arrived=arrived, onward=onward):
                arrived.wait_recv()
                onward.start()

            guarded(cond, pass_on)
            pending.append((onward, cond))

    def kv_finish(g):
        slot = kv.at[:, g * 8 + partner]
        cond = ((c == 1) | (s >= 4)) if g == 0 else s >= g
        guarded(cond, rcopy(slot, slot, p_s.at[g], p_r.at[g], {"exp": partner}).wait_recv)
        for dx in range(1, 4):
            sx = lax.rem(x + 4 - dx, 4)
            cond = ((sx < x) | (s >= 4)) if g == 0 else s >= g
            slot = kv.at[:, g * 8 + 2 * sx + 1 - c]
            guarded(
                cond, rcopy(slot, slot, f_s.at[g, dx], f_r.at[g, dx], {"exp": partner}).wait_recv
            )

    def kv_arrive(k):
        slot = kv.at[:, slot_of(k)]
        guarded(
            s >= k, rcopy(slot, slot, z_s.at[k - 1], z_r.at[k - 1], {"seq": prv}).wait_recv
        )
        if k < 4:
            send(kv_hop(k + 1), (s >= k) & (s < STEPS - 1))
        kv_across(0 if k == 4 else k, k)

    for d in range(1, CORES):
        to = lax.rem(e + d, CORES)
        send(rcopy(rows_in.at[to], disp.at[e], d_s.at[d], d_r.at[d], {"exp": to}))
    first, second = pl.ds(0, HALF), pl.ds(HALF, HALF)
    third, fourth = pl.ds(2 * HALF, HALF), pl.ds(3 * HALF, HALF)
    send(rcopy(gu_in.at[:, first], gu.at[:, third], g_s.at[0], g_r.at[0], to_a))
    send(rcopy(gu_in.at[:, second], gu.at[:, fourth], g_s.at[1], g_r.at[1], to_b))
    send(kv_hop(1), s < STEPS - 1)
    for d in range(1, CORES):
        to = lax.rem(e + d, CORES)
        send(rcopy(st_in.at[to], st_rx.at[e], sa_s.at[d], sa_r.at[d], {"exp": to}))
        send(rcopy(dec_in.at[to], dec_rx.at[e], da_s.at[d], da_r.at[d], {"exp": to}))
    kv_across(0, 0)
    send(rcopy(dn_in.at[first], dn.at[0, third], n_s.at[0], n_r.at[0], to_a))
    send(rcopy(dn_in.at[second], dn.at[0, fourth], n_s.at[1], n_r.at[1], to_b))
    send(rcopy(dn_in.at[second], dn.at[1, fourth], n_s.at[2], n_r.at[2], to_a))
    send(rcopy(dn_in.at[first], dn.at[1, third], n_s.at[3], n_r.at[3], to_b))
    own_gu = pltpu.make_async_copy(gu_in, gu.at[:, pl.ds(0, 2 * HALF)], l_s.at[0])
    own_dn = pltpu.make_async_copy(dn_in, dn.at[0, pl.ds(0, 2 * HALF)], l_s.at[1])
    own_gu.start()
    own_dn.start()
    kv[:, pl.ds(e, 1)] = kv_in[...][:, None]
    disp[pl.ds(e, 1)] = rows_in[pl.ds(e, 1)]
    st_rx[pl.ds(e, 1)] = st_in[pl.ds(e, 1)]
    dec_rx[pl.ds(e, 1)] = dec_in[pl.ds(e, 1)]
    h_all[...] = jnp.zeros_like(h_all)
    td_tx[...] = jnp.zeros_like(td_tx)

    kv_arrive(1)
    for d in range(1, CORES):
        frm = lax.rem(e + CORES - d, CORES)
        rcopy(disp.at[frm], disp.at[frm], d_s.at[d], d_r.at[d], {"exp": frm}).wait_recv()
    packed = jnp.dot(
        pack[...], disp[...].reshape(CORES * 2 * PAD, -1), preferred_element_type=F32
    ).astype(BF16)
    rows[pl.ds(s, 1)] = packed.reshape(1, 2, ROWS, -1)

    def rows_up(j, i):
        at = rows.at[lax.rem(s + STEPS - j, STEPS), i]
        return rcopy(at, at, rf_s.at[j, i], rf_r.at[j, i], {"seq": nxt})

    def rows_down(j, i):
        at = rows.at[lax.rem(s + j, STEPS), i]
        return rcopy(at, at, rb_s.at[j, i], rb_r.at[j, i], {"seq": prv})

    def rows_up_arrived(j, i):
        at = rows.at[lax.rem(s + STEPS - 1 - j, STEPS), i]
        return rcopy(at, at, rf_s.at[j, i], rf_r.at[j, i], {"seq": prv})

    def rows_down_arrived(j, i):
        at = rows.at[lax.rem(s + 1 + j, STEPS), i]
        return rcopy(at, at, rb_s.at[j, i], rb_r.at[j, i], {"seq": nxt})

    for i in range(2):
        send(rows_down(0, i))
        send(rows_up(0, i))
    kv_arrive(2)

    for d in range(1, CORES):
        frm = lax.rem(e + CORES - d, CORES)
        rcopy(st_rx.at[frm], st_rx.at[frm], sa_s.at[d], sa_r.at[d], {"exp": frm}).wait_recv()
        rcopy(dec_rx.at[frm], dec_rx.at[frm], da_s.at[d], da_r.at[d], {"exp": frm}).wait_recv()
    for h in range(2):
        part = slice(64 * h, 64 * h + 64)
        run = jnp.zeros((64, 128), F32)
        whole = jnp.ones((1, 128), F32)
        for k in range(CORES):
            inner[k, part, :] = run
            decay = dec_rx[k, h:h + 1, :]
            run = run * decay + st_rx[k, part, :].astype(F32)
            whole = whole * decay
        t_tx[part, :] = run.astype(BF16)
        td_tx[h:h + 1, :] = whole
    for d in range(1, STEPS):
        to = lax.rem(s + d, STEPS)
        send(rcopy(t_tx, t_rx.at[s], st_s.at[d], st_r.at[d], {"seq": to}), s + d < STEPS)
        send(rcopy(td_tx, td_rx.at[s], sd_s.at[d], sd_r.at[d], {"seq": to}), s + d < STEPS)

    kv_arrive(3)
    for d in range(1, STEPS):
        frm = lax.rem(s + STEPS - d, STEPS)
        at = t_rx.at[frm]
        guarded(d <= s, rcopy(at, at, st_s.at[d], st_r.at[d], {"seq": frm}).wait_recv)
        at = td_rx.at[frm]
        guarded(d <= s, rcopy(at, at, sd_s.at[d], sd_r.at[d], {"seq": frm}).wait_recv)
    carry[...] = jnp.zeros_like(carry)
    for k in range(STEPS - 1):

        def fold(k=k):
            for h in range(2):
                part = slice(64 * h, 64 * h + 64)
                carry[part, :] = carry[part, :] * td_rx[k, h:h + 1, :] + t_rx[
                    k, part, :
                ].astype(F32)

        pl.when(k < s)(fold)
    for h in range(2):
        part = slice(64 * h, 64 * h + 64)
        moved = carry[part, :]
        for k in range(CORES):
            ent_tx[k, part, :] = (inner[k, part, :] + moved).astype(BF16)
            moved = moved * dec_rx[k, h:h + 1, :]
    for d in range(1, CORES):
        to = lax.rem(e + d, CORES)
        send(rcopy(ent_tx.at[to], ent.at[e], se_s.at[d], se_r.at[d], {"exp": to}))
    ent[pl.ds(e, 1)] = ent_tx[pl.ds(e, 1)]
    kv_arrive(4)

    def to_mate_copy(b):
        return rcopy(h_all.at[b, 1 - t // 2], h_oth.at[b], h_s.at[b], h_r.at[b], to_mate)

    def expert_in(b):
        flat = rows[b].reshape(2 * ROWS, -1)
        nt = (((1,), (1,)), ((), ()))
        gated_part = lax.dot_general(flat, gu[0], nt, preferred_element_type=F32)
        up_part = lax.dot_general(flat, gu[1], nt, preferred_element_type=F32)
        units = (gated_part / (1.0 + jnp.exp(-gated_part)) * up_part).astype(BF16)
        h_all[b, 0, :, 0:UNITS] = units[0:ROWS]
        h_all[b, 1, :, 0:UNITS] = units[ROWS:2 * ROWS]
        to_mate_copy(b).start()

    def expert_pair(j):
        def one(i, _):
            expert_in(lax.rem(s + STEPS + (2 * i - 1) * (j + 1), STEPS))
            return 0

        lax.fori_loop(0, 2, one, 0)

    def rows_step(j):
        for i in range(2):
            rows_down_arrived(j, i).wait_recv()
            if j < 3:
                send(rows_down(j + 1, i))
            if j < 3:
                rows_up_arrived(j, i).wait_recv()
                if j < 2:
                    send(rows_up(j + 1, i))

    kv_forward(1)
    own_gu.wait()
    arrive_a = gu.at[:, third]
    arrive_b = gu.at[:, fourth]
    rcopy(arrive_a, arrive_a, g_s.at[0], g_r.at[0], to_a).wait_recv()
    rcopy(arrive_b, arrive_b, g_s.at[1], g_r.at[1], to_b).wait_recv()
    expert_in(s)
    rows_step(0)
    kv_forward(2)
    kv_forward(3)
    expert_pair(0)
    kv_forward(0)
    rows_step(1)
    at = dn.at[0, third]
    rcopy(at, at, n_s.at[0], n_r.at[0], to_a).wait_recv()
    send(rcopy(at, dn.at[1, first], n_s.at[4], n_r.at[4], to_b))
    at = dn.at[0, fourth]
    rcopy(at, at, n_s.at[1], n_r.at[1], to_b).wait_recv()
    send(rcopy(at, dn.at[1, second], n_s.at[5], n_r.at[5], to_a))
    expert_pair(1)
    rows_step(2)
    for g in (1, 2, 3, 0):
        kv_finish(g)
    attend_body(s, e, q, kv, heads)
    for d in range(1, CORES):
        frm = lax.rem(e + CORES - d, CORES)
        rcopy(ent.at[frm], ent.at[frm], se_s.at[d], se_r.at[d], {"exp": frm}).wait_recv()
    state_body(
        inputs, gate, inflow, readout, cum, cum_t, step_t, skip, gain, ent, state_out, gated
    )
    expert_pair(2)
    rows_step(3)
    expert_in(lax.rem(s + 4, STEPS))
    own_dn.wait()
    for n, at, dev in (
        (2, dn.at[1, fourth], to_a),
        (3, dn.at[1, third], to_b),
        (4, dn.at[1, first], to_b),
        (5, dn.at[1, second], to_a),
    ):
        rcopy(at, at, n_s.at[n], n_r.at[n], dev).wait_recv()
    for b in range(STEPS):
        to_mate_copy(b).wait()
    for copy, cond in pending:
        guarded(cond, copy.wait_send)


def spread(*operands):
    vm = pl.BlockSpec(memory_space=VM)
    hbm = pl.BlockSpec(memory_space=pl.ANY)
    width = operands[1].shape[-1]
    dma = pltpu.SemaphoreType.DMA
    return pl.pallas_call(
        spread_kernel,
        out_shape=(
            jax.ShapeDtypeStruct((2, 512, 128), BF16),
            jax.ShapeDtypeStruct((128, 1024), BF16),
            jax.ShapeDtypeStruct((STEPS, 2, ROWS, 512), BF16),
            jax.ShapeDtypeStruct((STEPS, ROWS, 512), BF16),
            jax.ShapeDtypeStruct((2, UNITS, width), BF16),
        ),
        in_specs=[vm] * 5 + [hbm] * 2 + [vm] * 10,
        out_specs=(vm,) * 5,
        scratch_shapes=[
            VM((2, UNITS, width), BF16),
            VM((4, 33, 128, 128), BF16),
            VM((STEPS, 2, ROWS, width), BF16),
            VM((CORES, 128, 128), BF16),
            VM((CORES, 2 * PAD, width), BF16),
            VM((CORES, 128, 128), BF16),
            VM((CORES, 8, 128), F32),
            VM((128, 128), BF16),
            VM((STEPS, 128, 128), BF16),
            VM((8, 128), F32),
            VM((STEPS, 8, 128), F32),
            VM((CORES, 128, 128), BF16),
            VM((CORES, 128, 128), F32),
            VM((128, 128), F32),
            VM((128, 512), F32),
            dma((2,)), dma((2,)), dma((2,)), dma((6,)), dma((6,)), dma((8,)), dma((8,)),
            dma((4,)), dma((4,)), dma((5, 4)), dma((4, 4)), dma((5,)), dma((4,)),
            dma((4, 4)), dma((4, 4)),
            dma((8,)), dma((8,)), dma((3, 2)), dma((3, 2)), dma((4, 2)), dma((4, 2)),
            dma((8,)), dma((8,)), dma((8,)), dma((8,)), dma((8,)), dma((8,)),
            dma((8,)), dma((8,)), dma((8,)), dma((8,)),
        ],
        compiler_params=pltpu.CompilerParams(
            collective_id=1, has_side_effects=True, vmem_limit_bytes=56 << 20
        ),
        name="spread",
    )(*operands)


def summary_kernel(inputs, inflow, weight_in, out):
    for pair in range(8):
        vectors = inflow[:, 128 * (pair // 4):128 * (pair // 4) + 128].astype(F32)
        both = inputs[:, 128 * pair:128 * pair + 128]
        for h in range(2):
            head = 2 * pair + h
            weighted = (weight_in[:, head:head + 1] * vectors).astype(BF16)
            res = lax.dot_general(
                both, weighted, (((0,), (0,)), ((), ())), preferred_element_type=F32
            )
            out[pair, 64 * h:64 * h + 64, :] = res[64 * h:64 * h + 64].astype(BF16)


def summary(inputs, inflow, weight_in):
    vm = pl.BlockSpec(memory_space=VM)
    return pl.pallas_call(
        summary_kernel,
        out_shape=jax.ShapeDtypeStruct((8, 128, 128), BF16),
        in_specs=[vm] * 3,
        out_specs=vm,
        cost_estimate=pl.CostEstimate(
            flops=1_000_000_000, bytes_accessed=1_000_000, transcendentals=0
        ),
        name="summary",
    )(inputs, inflow, weight_in)


def state_body(inputs, gate, inflow, readout, cum, cum_t, step_t, skip, gain, ent, out, gated):
    low = lax.broadcasted_iota(jnp.int32, (128, 128), 1) < 64
    causal = lax.broadcasted_iota(jnp.int32, (128, 128), 0) >= lax.broadcasted_iota(
        jnp.int32, (128, 128), 1)
    for g in range(2):
        cols = slice(128 * g, 128 * g + 128)
        read = readout[:, cols]
        rw = lax.dot_general(
            read, inflow[:, cols], (((1,), (1,)), ((), ())), preferred_element_type=F32
        )
        square = jnp.zeros((128, 1), F32)
        for p in range(4):
            pair = 4 * g + p
            at = slice(128 * pair, 128 * pair + 128)
            both = inputs[:, at]
            parts = []
            scales = []
            for h in range(2):
                head = 2 * pair + h
                own = cum[:, head:head + 1]
                gap = jnp.where(causal, own - cum_t[head:head + 1, :], 0.0)
                mixing = jnp.where(causal, jnp.exp(gap), 0.0) * rw * step_t[head:head + 1, :]
                parts.append(
                    jnp.dot(mixing.astype(BF16), both, preferred_element_type=F32)
                )
                scales.append(jnp.exp(own))
            intra = jnp.where(low, parts[0], parts[1])
            scale = jnp.where(low, scales[0], scales[1])
            inter = scale * lax.dot_general(
                read, ent[pair], (((1,), (1,)), ((), ())), preferred_element_type=F32
            )
            mixed = intra + inter + skip[:, at] * both.astype(F32)
            v = gate[:, at].astype(F32)
            value = mixed * (v / (1.0 + jnp.exp(-v)))
            gated[:, 128 * p:128 * p + 128] = value
            square = square + jnp.sum(value * value, axis=1, keepdims=True)
        inv = lax.rsqrt(square / 512.0 + EPSILON)
        wide = slice(512 * g, 512 * g + 512)
        out[:, wide] = (gated[...] * inv * gain[:, wide]).astype(BF16)


def gather_kernel(
    h_all, h_oth, dn, unpack, weigh, out,
    tx, rx, slots_tx, slots, mine_tx, mine,
    r_s, r_r, x_s, x_r, y_s, y_r,
):
    s = lax.axis_index("seq")
    e = lax.axis_index("exp")
    t = lax.axis_index("tp")
    nxt = lax.rem(s + 1, STEPS)
    prv = lax.rem(s + STEPS - 1, STEPS)
    greet(
        (
            ("exp", CORES, range(1, CORES)),
            ("seq", STEPS, (1, STEPS - 1)),
            ("tp", TPS, range(1, TPS)),
        )
    )
    pending = []
    width = dn.shape[-1] // 4

    def columns(stream):
        return slice(width * stream, width * stream + width)

    def ring(stream, j):
        to = nxt if stream < 2 else prv
        return rcopy(
            tx.at[stream, j], rx.at[stream, j], r_s.at[stream, j], r_r.at[stream, j], {"seq": to}
        )

    def owner(stream, j):
        if stream < 2:
            return lax.rem(s + 2 * STEPS - 1 - j, STEPS)
        return lax.rem(s + 1 + j, STEPS)

    def partial_of(q, half):
        cols = slice(2 * width * half, 2 * width * (half + 1))
        return jnp.dot(
            h_all[q, t // 2, :, 0:UNITS], dn[0, :, cols], preferred_element_type=F32
        ) + jnp.dot(h_oth[q, :, 0:UNITS], dn[1, :, cols], preferred_element_type=F32)

    for j in range(STEPS - 1):
        for half in range(2):
            value = partial_of(owner(2 * half, j), half)
            for i in range(2):
                stream = 2 * half + i
                piece = value[:, columns(i)]
                if j > 0:
                    ring(stream, j - 1).wait_recv()
                    piece = piece + rx[stream, j - 1].astype(F32)
                tx[stream, j] = piece.astype(BF16)
                copy = ring(stream, j)
                copy.start()
                pending.append(copy)
    for half in range(2):
        value = partial_of(s, half)
        for i in range(2):
            stream = 2 * half + i
            ring(stream, STEPS - 2).wait_recv()
            total = value[:, columns(i)] + rx[stream, STEPS - 2].astype(F32)
            spaced = jnp.dot(unpack[...], total.astype(BF16), preferred_element_type=F32)
            slots_tx[:, :, columns(stream)] = spaced.astype(BF16).reshape(CORES, PAD, width)
    for d in range(1, CORES):
        to = lax.rem(e + d, CORES)
        copy = rcopy(slots_tx.at[to], slots.at[e], x_s.at[d], x_r.at[d], {"exp": to})
        copy.start()
        pending.append(copy)
    slots[pl.ds(e, 1)] = slots_tx[pl.ds(e, 1)]
    for d in range(1, CORES):
        frm = lax.rem(e + CORES - d, CORES)
        at = slots.at[frm]
        rcopy(at, at, x_s.at[d], x_r.at[d], {"exp": frm}).wait_recv()
    high = weigh[...].astype(BF16)
    rest = (weigh[...] - high.astype(F32)).astype(BF16)
    for quarter in range(TPS):
        at = slots[:, :, columns(quarter)].reshape(CORES * PAD, width)
        mine_tx[quarter] = (
            jnp.dot(high, at, preferred_element_type=F32)
            + jnp.dot(rest, at, preferred_element_type=F32)
        ).astype(BF16)
    for d in range(1, TPS):
        to = lax.rem(t + d, TPS)
        copy = rcopy(mine_tx.at[to], mine.at[d], y_s.at[d], y_r.at[d], {"tp": to})
        copy.start()
        pending.append(copy)
    total = mine_tx[t].astype(F32)
    for d in range(1, TPS):
        frm = lax.rem(t + TPS - d, TPS)
        at = mine.at[d]
        rcopy(at, at, y_s.at[d], y_r.at[d], {"tp": frm}).wait_recv()
        total = total + mine[d].astype(F32)
    out[...] = total.astype(BF16)
    for copy in pending:
        copy.wait_send()


def gathered(h_all, h_oth, dn, unpack, weigh):
    vm = pl.BlockSpec(memory_space=VM)
    width = dn.shape[-1]
    q = width // 4
    dma = pltpu.SemaphoreType.DMA
    return pl.pallas_call(
        gather_kernel,
        out_shape=jax.ShapeDtypeStruct((128, q), BF16),
        in_specs=[vm] * 5,
        out_specs=vm,
        scratch_shapes=[
            VM((4, STEPS - 1, ROWS, q), BF16),
            VM((4, STEPS - 1, ROWS, q), BF16),
            VM((CORES, PAD, width), BF16),
            VM((CORES, PAD, width), BF16),
            VM((TPS, 128, q), BF16),
            VM((TPS, 128, q), BF16),
            dma((4, STEPS - 1)), dma((4, STEPS - 1)), dma((8,)), dma((8,)), dma((4,)), dma((4,)),
        ],
        compiler_params=pltpu.CompilerParams(
            collective_id=2, has_side_effects=True, vmem_limit_bytes=40 << 20
        ),
        name="collect",
    )(h_all, h_oth, dn, unpack, weigh)


def local(
    query_heads, key_heads, value_head_rows, state_input, state_gate, state_inflow,
    state_readout, step_size, log_decay, skip_scale, state_gain, hidden_in, mlp_gain,
    router_weight, expert_ids, slot_index, gate_up, down_proj,
):
    tp = lax.axis_index("tp")
    hidden = hidden_in.astype(F32)
    mean_square = jnp.mean(hidden * hidden, axis=-1, keepdims=True)
    normed = (hidden * lax.rsqrt(mean_square + EPSILON) * mlp_gain).astype(BF16)
    gate_values = jax.nn.sigmoid(jnp.dot(normed, router_weight, preferred_element_type=F32))
    one_hot = expert_ids[..., None] == jnp.arange(EXPERTS, dtype=jnp.int32)
    chosen = jnp.sum(jnp.where(one_hot, gate_values[:, None, :], 0.0), axis=-1)
    mixing = chosen / jnp.sum(chosen, axis=1, keepdims=True)
    is_live = slot_index >= 0
    quarter = slot_index // QUARTER
    inside = slot_index - quarter * QUARTER
    lanes = jnp.arange(EXPERTS * 2 * PAD, dtype=jnp.int32)
    near = is_live & (quarter % 2 == tp % 2)
    place = jnp.where(near, expert_ids * (2 * PAD) + (quarter // 2) * PAD + inside, -1)
    picker = jnp.any(place[..., None] == lanes, axis=1).astype(BF16)
    outgoing = lax.dot_general(
        picker, normed, (((0,), (0,)), ((), ())), preferred_element_type=F32
    ).astype(BF16).reshape(EXPERTS, 2 * PAD, -1)
    home = jnp.where(is_live & (quarter == tp), expert_ids * PAD + inside, -1)
    hits = home[..., None] == lanes[:EXPERTS * PAD]
    weigh = jnp.sum(jnp.where(hits, mixing[..., None], 0.0), axis=1)
    flat = jnp.arange(2 * ROWS)
    source = (flat % ROWS) // QUARTER * (2 * PAD) + flat // ROWS * PAD + flat % QUARTER
    pack = (source[:, None] == lanes[None]).astype(BF16)
    flat = jnp.arange(ROWS)
    unpack = (
        (flat // QUARTER * PAD + flat % QUARTER)[None] == jnp.arange(CORES * PAD)[:, None]
    ).astype(BF16)

    cum = jnp.cumsum(log_decay, axis=0)
    block_total = cum[-1]
    weight_in = jnp.exp(block_total[None] - cum) * step_size
    states = summary(state_input, state_inflow.reshape(128, 256), weight_in)
    decays = jnp.pad(jnp.exp(block_total).reshape(CORES, 2), ((0, 0), (0, 6)))
    decays = jnp.broadcast_to(decays[..., None], (CORES, 8, 128))
    kv_in = jnp.concatenate(
        [jnp.transpose(key_heads, (1, 0, 2)), jnp.transpose(value_head_rows, (1, 0, 2))], axis=0
    )
    heads, state_out, h_all, h_oth, down = spread(
        kv_in, outgoing, pack, states, decays,
        jnp.transpose(gate_up[0], (1, 0, 2)), down_proj[0],
        jnp.transpose(query_heads, (1, 0, 2)).reshape(2, 512, 128),
        state_input, state_gate, state_inflow.reshape(128, 256), state_readout.reshape(128, 256),
        cum, cum.T, step_size.T, jnp.repeat(skip_scale, 64)[None], state_gain[None],
    )
    window_out = jnp.transpose(heads.reshape(8, 128, 128), (1, 0, 2))
    routed_out = gathered(h_all, h_oth, down, unpack, weigh)
    return window_out, state_out, routed_out


def solution(mesh):
    both = ("seq", "exp")
    placed = (
        P(both, "tp", None), P(both, "tp", None), P(both, "tp", None),
        P(both, "tp"), P(both, "tp"), P(both, "tp", None), P(both, "tp", None),
        P(both, "tp"), P(both, "tp"), P("tp"), P("tp"), P(both, None), P(), P(),
        P(both, None), P(both, None),
        P("exp", ("seq", "tp"), None, None), P("exp", ("seq", "tp"), None),
    )
    return jax.shard_map(
        local,
        mesh=mesh,
        in_specs=placed,
        out_specs=(P(both, "tp", None), P(both, "tp"), P(both, "tp")),
        check_vma=False,
    )
```

```python
import functools
import math

import jax
import jax.numpy as jnp
from jax import lax
from jax.experimental import pallas as pl
from jax.experimental.pallas import tpu as pltpu
from jax.sharding import PartitionSpec as P

EXPERTS = 8
CAP = 40
STEPS = 8
CORES = 8
TPS = 4
QUARTER = 10
PAD = 16
ROWS = 80
UNITS = 448
HALF = 112
EPSILON = 1e-05
VM = pltpu.VMEM
MESH = pl.DeviceIdType.MESH
F32 = jnp.float32
BF16 = jnp.bfloat16


def rcopy(src, dst, ss, rs, dev):
    return pltpu.make_async_remote_copy(
        src_ref=src, dst_ref=dst, send_sem=ss, recv_sem=rs, device_id=dev, device_id_type=MESH
    )


def guarded(cond, fn):
    if cond is True:
        fn()
    else:
        pl.when(cond)(fn)


def greet(groups):
    barrier = pltpu.get_barrier_semaphore()
    count = 0
    for axis, size, shifts in groups:
        me = lax.axis_index(axis)
        for d in shifts:
            pl.semaphore_signal(
                barrier, inc=1, device_id={axis: lax.rem(me + d, size)}, device_id_type=MESH
            )
            count += 1
    pl.semaphore_wait(barrier, count)


def attend_body(s, e, q, kv, out, group):
    row = lax.rem(lax.broadcasted_iota(jnp.int32, (512, 1024), 0), 128)
    col = lax.broadcasted_iota(jnp.int32, (512, 1024), 1)
    place = col // 128
    inside = lax.rem(col, 128)
    far_ok = s >= 4
    near = (place < e) | ((place == e) & (inside <= row)) | ((place > e) & far_ok)
    vrow = lax.broadcasted_iota(jnp.int32, (1024, 128), 0) // 128
    v_ok = (vrow <= e) | far_ok
    last = (
        lax.broadcasted_iota(jnp.int32, (512, 128), 1)
        > lax.rem(lax.broadcasted_iota(jnp.int32, (512, 128), 0), 128)
    ) & far_ok
    scale = 1.0 / math.sqrt(128) * math.log2(math.e)

    def chunk(carried, query, keys, values, mask):
        top, total, acc = carried
        scores = lax.dot_general(
            query, keys, (((1,), (1,)), ((), ())), preferred_element_type=F32
        )
        if mask is not None:
            scores = jnp.where(mask, scores, -1e30)
        new = jnp.maximum(top, jnp.max(scores, axis=1, keepdims=True))
        weights = jnp.exp2((scores - new) * scale)
        if mask is not None:
            weights = jnp.where(mask, weights, 0.0)
        factor = jnp.exp2((top - new) * scale)
        total = total * factor + jnp.sum(weights, axis=1, keepdims=True)
        acc = acc * factor + jnp.dot(
            weights.astype(BF16), values, preferred_element_type=F32
        )
        return new, total, acc

    query = q[group]
    k0 = kv[group, 0:8].reshape(1024, 128)
    v0 = jnp.where(v_ok, kv[2 + group, 0:8].reshape(1024, 128), jnp.zeros((), BF16))
    state = (
        jnp.full((512, 1), -1e30, F32),
        jnp.zeros((512, 1), F32),
        jnp.zeros((512, 128), F32),
    )
    state = chunk(state, query, k0, v0, near)
    vl = jnp.where(far_ok, kv[2 + group, 32], jnp.zeros((), BF16))
    state = chunk(state, query, kv[group, 32], vl, last)

    def more(k, carried):
        keys = kv[group, pl.ds(k * 8, 8)].reshape(1024, 128)
        values = kv[2 + group, pl.ds(k * 8, 8)].reshape(1024, 128)
        return chunk(carried, query, keys, values, None)

    _, total, acc = lax.fori_loop(1, jnp.minimum(s, 3) + 1, more, state)
    out[group] = (acc / total).astype(BF16)


def spread_kernel(
    kv_in, hidden, mlp_gain, router_t, ints, gu_in, dn_in, q,
    inputs, gate, inflow, readout, decay_t, step_t, skip, gain,
    heads, state_out, routed,
    h_all, h_oth, dn, rows_in, st_in, dec_in, weigh, cum, cum_t,
    tx_f, rx_f, tx_b, rx_b, slots_tx, slots, mine_tx, mine,
    gu, kv, rows, ent, disp, st_rx, dec_rx, t_tx, t_rx, td_tx, td_rx, ent_tx, inner, carry, gated,
    qf_s, qf_r, qb_s, qb_r, o_s, o_r, y_s, y_r,
    l_s, g_s, g_r, n_s, n_r, h_s, h_r,
    z_s, z_r, x_s, x_r, p_s, p_r, f_s, f_r,
    d_s, d_r, rf_s, rf_r, rb_s, rb_r, sa_s, sa_r, da_s, da_r, st_s, st_r, sd_s, sd_r, se_s, se_r,
):
    s = lax.axis_index("seq")
    e = lax.axis_index("exp")
    t = lax.axis_index("tp")
    x = e // 2
    c = lax.rem(e, 2)
    partner = e + 1 - 2 * c
    nxt = lax.rem(s + 1, STEPS)
    prv = lax.rem(s + STEPS - 1, STEPS)
    odd = lax.rem(t, 2)
    to_a = {"tp": t + 1 - 2 * odd}
    to_b = {"tp": lax.rem(t + 3 + 2 * odd, TPS)}
    to_mate = {"tp": lax.rem(t + 2, TPS)}
    greet(
        (
            ("tp", TPS, range(1, TPS)),
            ("exp", CORES, range(1, CORES)),
            ("seq", STEPS, range(1, STEPS)),
        )
    )
    pending = []

    def send(copy, cond=True):
        guarded(cond, copy.start)
        pending.append((copy, cond))

    def slot_of(k):
        return 32 if k == 4 else k * 8 + e

    def block(k):
        return kv_in if k == 0 else kv.at[:, slot_of(k)]

    def kv_hop(k):
        return rcopy(
            block(k - 1), kv.at[:, slot_of(k)], z_s.at[k - 1], z_r.at[k - 1], {"seq": nxt}
        )

    def kv_across(g, k):
        for dx in range(1, 4):
            tx = lax.rem(x + dx, 4)
            if k == 0:
                cond = tx > x
            elif k == 4:
                cond = (tx < x) & (s >= 4)
            else:
                cond = s >= k
            send(
                rcopy(
                    block(k), kv.at[:, g * 8 + e], x_s.at[k, dx], x_r.at[g, dx],
                    {"exp": 2 * tx + c},
                ),
                cond,
            )
        if k == 0:
            cond = c == 0
        elif k == 4:
            cond = (c == 1) & (s >= 4)
        else:
            cond = s >= k
        send(
            rcopy(block(k), kv.at[:, g * 8 + e], p_s.at[k], p_r.at[g], {"exp": partner}), cond
        )

    def kv_forward(g):
        for dx in range(1, 4):
            sx = lax.rem(x + 4 - dx, 4)
            cond = ((sx < x) | (s >= 4)) if g == 0 else s >= g
            slot = kv.at[:, g * 8 + 2 * sx + c]
            arrived = rcopy(slot, slot, x_s.at[g, dx], x_r.at[g, dx], {"exp": 2 * sx + c})
            onward = rcopy(slot, slot, f_s.at[g, dx], f_r.at[g, dx], {"exp": partner})

            def pass_on(arrived=arrived, onward=onward):
                arrived.wait_recv()
                onward.start()

            guarded(cond, pass_on)
            pending.append((onward, cond))

    def kv_finish(g):
        slot = kv.at[:, g * 8 + partner]
        cond = ((c == 1) | (s >= 4)) if g == 0 else s >= g
        guarded(cond, rcopy(slot, slot, p_s.at[g], p_r.at[g], {"exp": partner}).wait_recv)
        for dx in range(1, 4):
            sx = lax.rem(x + 4 - dx, 4)
            cond = ((sx < x) | (s >= 4)) if g == 0 else s >= g
            slot = kv.at[:, g * 8 + 2 * sx + 1 - c]
            guarded(
                cond, rcopy(slot, slot, f_s.at[g, dx], f_r.at[g, dx], {"exp": partner}).wait_recv
            )

    def kv_arrive(k):
        slot = kv.at[:, slot_of(k)]
        guarded(
            s >= k, rcopy(slot, slot, z_s.at[k - 1], z_r.at[k - 1], {"seq": prv}).wait_recv
        )
        if k < 4:
            send(kv_hop(k + 1), (s >= k) & (s < STEPS - 1))
        kv_across(0 if k == 4 else k, k)

    first, second = pl.ds(0, HALF), pl.ds(HALF, HALF)
    third, fourth = pl.ds(2 * HALF, HALF), pl.ds(3 * HALF, HALF)
    send(rcopy(gu_in.at[:, first], gu.at[:, third], g_s.at[0], g_r.at[0], to_a))
    send(rcopy(gu_in.at[:, second], gu.at[:, fourth], g_s.at[1], g_r.at[1], to_b))
    send(kv_hop(1), s < STEPS - 1)
    send(rcopy(dn_in.at[first], dn.at[0, third], n_s.at[0], n_r.at[0], to_a))
    send(rcopy(dn_in.at[second], dn.at[0, fourth], n_s.at[1], n_r.at[1], to_b))
    send(rcopy(dn_in.at[second], dn.at[1, fourth], n_s.at[2], n_r.at[2], to_a))
    send(rcopy(dn_in.at[first], dn.at[1, third], n_s.at[3], n_r.at[3], to_b))
    own_gu = pltpu.make_async_copy(gu_in, gu.at[:, pl.ds(0, 2 * HALF)], l_s.at[0])
    own_dn = pltpu.make_async_copy(dn_in, dn.at[0, pl.ds(0, 2 * HALF)], l_s.at[1])
    own_gu.start()
    own_dn.start()
    h_all[...] = jnp.zeros_like(h_all)
    wide = hidden[...].astype(F32)
    level = lax.rsqrt(jnp.mean(wide * wide, axis=1, keepdims=True) + EPSILON)
    normed = (wide * level * mlp_gain[...]).astype(BF16)
    lanes = lax.broadcasted_iota(jnp.int32, (128, CORES * 2 * PAD), 1)
    picker = ((ints[:, 0:1] == lanes) | (ints[:, 1:2] == lanes)).astype(F32).astype(BF16)
    rows_in[...] = lax.dot_general(
        picker, normed, (((0,), (0,)), ((), ())), preferred_element_type=F32
    ).astype(BF16).reshape(CORES, 2, PAD, -1)
    for i in range(2):
        for d in range(1, CORES):
            to = lax.rem(e + d, CORES)
            send(rcopy(rows_in.at[to, i], disp.at[i, e], d_s.at[i, d], d_r.at[i, d], {"exp": to}))
        disp[i, pl.ds(e, 1)] = rows_in[pl.ds(e, 1), i]

    exact = lax.Precision.HIGHEST
    low_tri = (
        lax.broadcasted_iota(jnp.int32, (128, 128), 0)
        >= lax.broadcasted_iota(jnp.int32, (128, 128), 1)
    ).astype(F32)
    eye = (
        lax.broadcasted_iota(jnp.int32, (128, 128), 0)
        == lax.broadcasted_iota(jnp.int32, (128, 128), 1)
    ).astype(F32)
    both_last = (((1,), (1,)), ((), ()))
    cum[...] = lax.dot_general(
        low_tri, decay_t[...], both_last, precision=exact, preferred_element_type=F32
    )
    cum_t[...] = lax.dot_general(
        decay_t[...], low_tri, both_last, precision=exact, preferred_element_type=F32
    )
    block_total = cum_t[:, 127:128]
    weight_t = jnp.exp(block_total - cum_t[...]) * step_t[...]
    weight_in = lax.dot_general(
        eye, weight_t, both_last, precision=exact, preferred_element_type=F32
    )
    whole_decay = jnp.broadcast_to(jnp.exp(block_total), (16, 128))
    dec_in[...] = jnp.zeros_like(dec_in)
    for pair in range(8):
        dec_in[pair, 0:2, :] = whole_decay[2 * pair:2 * pair + 2]
        vectors = inflow[:, 128 * (pair // 4):128 * (pair // 4) + 128].astype(F32)
        both = inputs[:, 128 * pair:128 * pair + 128]
        for h in range(2):
            head = 2 * pair + h
            weighted = (weight_in[:, head:head + 1] * vectors).astype(BF16)
            res = lax.dot_general(
                both, weighted, (((0,), (0,)), ((), ())), preferred_element_type=F32
            )
            st_in[pair, 64 * h:64 * h + 64, :] = res[64 * h:64 * h + 64].astype(BF16)
    for d in range(1, CORES):
        to = lax.rem(e + d, CORES)
        send(rcopy(st_in.at[to], st_rx.at[e], sa_s.at[d], sa_r.at[d], {"exp": to}))
        send(rcopy(dec_in.at[to], dec_rx.at[e], da_s.at[d], da_r.at[d], {"exp": to}))
    kv_across(0, 0)
    kv[:, pl.ds(e, 1)] = kv_in[...][:, None]
    st_rx[pl.ds(e, 1)] = st_in[pl.ds(e, 1)]
    dec_rx[pl.ds(e, 1)] = dec_in[pl.ds(e, 1)]
    td_tx[...] = jnp.zeros_like(td_tx)
    lane = lax.broadcasted_iota(jnp.int32, (ROWS, CORES * PAD), 1)
    place = (lane // PAD) * QUARTER + lax.rem(lane, PAD)
    fits = lax.rem(lane, PAD) < QUARTER
    pack = (
        (place == lax.broadcasted_iota(jnp.int32, (ROWS, CORES * PAD), 0)) & fits
    ).astype(F32).astype(BF16)

    kv_arrive(1)

    def rows_up(j, i):
        at = rows.at[lax.rem(s + STEPS - j, STEPS), i]
        return rcopy(at, at, rf_s.at[j, i], rf_r.at[j, i], {"seq": nxt})

    def rows_down(j, i):
        at = rows.at[lax.rem(s + j, STEPS), i]
        return rcopy(at, at, rb_s.at[j, i], rb_r.at[j, i], {"seq": prv})

    def rows_up_arrived(j, i):
        at = rows.at[lax.rem(s + STEPS - 1 - j, STEPS), i]
        return rcopy(at, at, rf_s.at[j, i], rf_r.at[j, i], {"seq": prv})

    def rows_down_arrived(j, i):
        at = rows.at[lax.rem(s + 1 + j, STEPS), i]
        return rcopy(at, at, rb_s.at[j, i], rb_r.at[j, i], {"seq": nxt})

    for i in range(2):
        for d in range(1, CORES):
            frm = lax.rem(e + CORES - d, CORES)
            at = disp.at[i, frm]
            rcopy(at, at, d_s.at[i, d], d_r.at[i, d], {"exp": frm}).wait_recv()
        rows[pl.ds(s, 1), i] = jnp.dot(
            pack, disp[i].reshape(CORES * PAD, -1), preferred_element_type=F32
        ).astype(BF16)[None]
        send(rows_down(0, i))
        send(rows_up(0, i))
        if i == 0:
            logits = lax.dot_general(
                normed, router_t[...], both_last, preferred_element_type=F32
            )
            gates = 1.0 / (1.0 + jnp.exp(-logits))
            expert = lax.broadcasted_iota(jnp.int32, (128, EXPERTS), 1)
            chosen = [
                jnp.sum(jnp.where(ints[:, 4 + k:5 + k] == expert, gates, 0.0), axis=1,
                        keepdims=True)
                for k in range(2)
            ]
            home = lax.broadcasted_iota(jnp.int32, (128, CORES * PAD), 1)
            weigh[...] = sum(
                jnp.where(ints[:, 2 + k:3 + k] == home, chosen[k] / (chosen[0] + chosen[1]), 0.0)
                for k in range(2)
            )
            kv_arrive(2)

    for d in range(1, CORES):
        frm = lax.rem(e + CORES - d, CORES)
        rcopy(st_rx.at[frm], st_rx.at[frm], sa_s.at[d], sa_r.at[d], {"exp": frm}).wait_recv()
        rcopy(dec_rx.at[frm], dec_rx.at[frm], da_s.at[d], da_r.at[d], {"exp": frm}).wait_recv()
    for h in range(2):
        part = slice(64 * h, 64 * h + 64)
        run = jnp.zeros((64, 128), F32)
        whole = jnp.ones((1, 128), F32)
        for k in range(CORES):
            inner[k, part, :] = run
            decay = dec_rx[k, h:h + 1, :]
            run = run * decay + st_rx[k, part, :].astype(F32)
            whole = whole * decay
        t_tx[part, :] = run.astype(BF16)
        td_tx[h:h + 1, :] = whole
    for d in range(1, STEPS):
        to = lax.rem(s + d, STEPS)
        send(rcopy(t_tx, t_rx.at[s], st_s.at[d], st_r.at[d], {"seq": to}), s + d < STEPS)
        send(rcopy(td_tx, td_rx.at[s], sd_s.at[d], sd_r.at[d], {"seq": to}), s + d < STEPS)

    kv_arrive(3)
    for d in range(1, STEPS):
        frm = lax.rem(s + STEPS - d, STEPS)
        at = t_rx.at[frm]
        guarded(d <= s, rcopy(at, at, st_s.at[d], st_r.at[d], {"seq": frm}).wait_recv)
        at = td_rx.at[frm]
        guarded(d <= s, rcopy(at, at, sd_s.at[d], sd_r.at[d], {"seq": frm}).wait_recv)
    carry[...] = jnp.zeros_like(carry)
    for k in range(STEPS - 1):

        def fold(k=k):
            for h in range(2):
                part = slice(64 * h, 64 * h + 64)
                carry[part, :] = carry[part, :] * td_rx[k, h:h + 1, :] + t_rx[
                    k, part, :
                ].astype(F32)

        pl.when(k < s)(fold)
    for h in range(2):
        part = slice(64 * h, 64 * h + 64)
        moved = carry[part, :]
        for k in range(CORES):
            ent_tx[k, part, :] = (inner[k, part, :] + moved).astype(BF16)
            moved = moved * dec_rx[k, h:h + 1, :]
    for d in range(1, CORES):
        to = lax.rem(e + d, CORES)
        send(rcopy(ent_tx.at[to], ent.at[e], se_s.at[d], se_r.at[d], {"exp": to}))
    ent[pl.ds(e, 1)] = ent_tx[pl.ds(e, 1)]
    kv_arrive(4)

    def to_mate_copy(b):
        return rcopy(h_all.at[b, 1 - t // 2], h_oth.at[b], h_s.at[b], h_r.at[b], to_mate)

    def expert_in(b):
        flat = rows[b].reshape(2 * ROWS, -1)
        nt = (((1,), (1,)), ((), ()))
        gated_part = lax.dot_general(flat, gu[0], nt, preferred_element_type=F32)
        up_part = lax.dot_general(flat, gu[1], nt, preferred_element_type=F32)
        units = (gated_part / (1.0 + jnp.exp(-gated_part)) * up_part).astype(BF16)
        h_all[b, 0, :, 0:UNITS] = units[0:ROWS]
        h_all[b, 1, :, 0:UNITS] = units[ROWS:2 * ROWS]
        to_mate_copy(b).start()

    def expert_pair(j):
        def one(i, _):
            expert_in(lax.rem(s + STEPS + (2 * i - 1) * (j + 1), STEPS))
            return 0

        lax.fori_loop(0, 2, one, 0)

    def rows_step(j):
        for i in range(2):
            rows_down_arrived(j, i).wait_recv()
            if j < 3:
                send(rows_down(j + 1, i))
            if j < 3:
                rows_up_arrived(j, i).wait_recv()
                if j < 2:
                    send(rows_up(j + 1, i))

    kv_forward(1)
    own_gu.wait()
    arrive_a = gu.at[:, third]
    arrive_b = gu.at[:, fourth]
    rcopy(arrive_a, arrive_a, g_s.at[0], g_r.at[0], to_a).wait_recv()
    rcopy(arrive_b, arrive_b, g_s.at[1], g_r.at[1], to_b).wait_recv()
    expert_in(s)
    rows_step(0)
    kv_forward(2)
    kv_forward(3)
    expert_pair(0)
    kv_forward(0)
    rows_step(1)
    at = dn.at[0, third]
    rcopy(at, at, n_s.at[0], n_r.at[0], to_a).wait_recv()
    send(rcopy(at, dn.at[1, first], n_s.at[4], n_r.at[4], to_b))
    at = dn.at[0, fourth]
    rcopy(at, at, n_s.at[1], n_r.at[1], to_b).wait_recv()
    send(rcopy(at, dn.at[1, second], n_s.at[5], n_r.at[5], to_a))
    expert_pair(1)
    for g in (1, 2, 3, 0):
        kv_finish(g)
    attend_body(s, e, q, kv, heads, 0)
    rows_step(2)
    expert_pair(2)
    attend_body(s, e, q, kv, heads, 1)
    for d in range(1, CORES):
        frm = lax.rem(e + CORES - d, CORES)
        rcopy(ent.at[frm], ent.at[frm], se_s.at[d], se_r.at[d], {"exp": frm}).wait_recv()
    state_body(
        inputs, gate, inflow, readout, cum, cum_t, step_t, skip, gain, ent, state_out, gated
    )
    own_dn.wait()
    for n, at, dev in (
        (2, dn.at[1, fourth], to_a),
        (3, dn.at[1, third], to_b),
        (4, dn.at[1, first], to_b),
        (5, dn.at[1, second], to_a),
    ):
        rcopy(at, at, n_s.at[n], n_r.at[n], dev).wait_recv()

    width = dn.shape[-1] // 4

    def columns(stream):
        return slice(width * stream, width * stream + width)

    def mate_arrived(b):
        to_mate_copy(b).wait_recv()

    def partial_of(b, half):
        cols = slice(2 * width * half, 2 * width * (half + 1))
        return jnp.dot(
            h_all[b, t // 2, :, 0:UNITS], dn[0, :, cols], preferred_element_type=F32
        ) + jnp.dot(h_oth[b, :, 0:UNITS], dn[1, :, cols], preferred_element_type=F32)

    def up(stream, j):
        return rcopy(
            tx_f.at[stream, j], rx_f.at[stream, j], qf_s.at[stream, j], qf_r.at[stream, j],
            {"seq": nxt},
        )

    def down(stream, j):
        return rcopy(
            tx_b.at[stream, j], rx_b.at[stream, j], qb_s.at[stream, j], qb_r.at[stream, j],
            {"seq": prv},
        )

    def hop(half, j, rising, value):
        begin = 0 if (half == 0) == rising else 1
        tx, rx, line = (tx_f, rx_f, up) if rising else (tx_b, rx_b, down)
        for i in range(2):
            stream = 2 * half + i
            piece = value[:, columns(i)]
            if j > begin:
                line(stream, j - 1).wait_recv()
                piece = piece + rx[stream, j - 1].astype(F32)
            tx[stream, j] = piece.astype(BF16)
            send(line(stream, j))

    def ahead(d):
        return lax.rem(s + d, STEPS)

    def short_hop(j):
        hop(1, j, True, partial_of(ahead(4 - j), 1))
        hop(0, j, False, partial_of(ahead(4 + j), 0))

    def long_hop(j):
        hop(0, j, True, partial_of(ahead(4 - j), 0))
        hop(1, j, False, partial_of(ahead(4 + j), 1))

    mate_arrived(ahead(3))
    mate_arrived(ahead(5))
    short_hop(1)
    rows_step(3)
    expert_in(ahead(4))
    for d in (2, 6, 1, 7, 0):
        mate_arrived(ahead(d))
    short_hop(2)
    mate_arrived(ahead(4))
    long_hop(0)
    short_hop(3)
    for j in range(1, 4):
        long_hop(j)
    finals = [partial_of(s, half) for half in range(2)]

    def slot_copy(stream, d, there):
        return rcopy(
            slots_tx.at[stream, there], slots.at[stream, e], o_s.at[stream, d],
            o_r.at[stream, d], {"exp": there},
        )

    for stream in (0, 2, 1, 3):
        half, i = stream // 2, stream % 2
        up(stream, 3).wait_recv()
        down(stream, 3).wait_recv()
        total = (
            finals[half][:, columns(i)]
            + rx_f[stream, 3].astype(F32)
            + rx_b[stream, 3].astype(F32)
        )
        spaced = lax.dot_general(
            pack, total.astype(BF16), (((0,), (0,)), ((), ())), preferred_element_type=F32
        )
        slots_tx[stream] = spaced.astype(BF16).reshape(CORES, PAD, width)
        for d in range(1, CORES):
            send(slot_copy(stream, d, lax.rem(e + d, CORES)))
        slots[stream, pl.ds(e, 1)] = slots_tx[stream, pl.ds(e, 1)]
    high = weigh[...].astype(BF16)
    rest = (weigh[...] - high.astype(F32)).astype(BF16)
    for stream in (0, 2, 1, 3):
        for d in range(1, CORES):
            frm = lax.rem(e + CORES - d, CORES)
            at = slots.at[stream, frm]
            rcopy(at, at, o_s.at[stream, d], o_r.at[stream, d], {"exp": frm}).wait_recv()
        at = slots[stream].reshape(CORES * PAD, width)
        mine_tx[stream] = (
            jnp.dot(high, at, preferred_element_type=F32)
            + jnp.dot(rest, at, preferred_element_type=F32)
        ).astype(BF16)
        send(
            rcopy(mine_tx.at[stream], mine.at[t], y_s.at[stream], y_r.at[t], {"tp": stream}),
            t != stream,
        )
    total = mine_tx[t].astype(F32)
    for d in range(1, TPS):
        frm = lax.rem(t + TPS - d, TPS)
        at = mine.at[frm]
        rcopy(at, at, y_s.at[frm], y_r.at[frm], {"tp": frm}).wait_recv()
        total = total + mine[frm].astype(F32)
    routed[...] = total.astype(BF16)
    for b in range(STEPS):
        to_mate_copy(b).wait_send()
    for copy, cond in pending:
        guarded(cond, copy.wait_send)


def spread(*operands):
    vm = pl.BlockSpec(memory_space=VM)
    hbm = pl.BlockSpec(memory_space=pl.ANY)
    width = operands[1].shape[-1]
    quarter = width // 4
    dma = pltpu.SemaphoreType.DMA
    return pl.pallas_call(
        spread_kernel,
        out_shape=(
            jax.ShapeDtypeStruct((2, 512, 128), BF16),
            jax.ShapeDtypeStruct((128, 1024), BF16),
            jax.ShapeDtypeStruct((128, quarter), BF16),
        ),
        in_specs=[vm] * 5 + [hbm] * 2 + [vm] * 9,
        out_specs=(vm,) * 3,
        scratch_shapes=[
            VM((STEPS, 2, ROWS, 512), BF16),
            VM((STEPS, ROWS, 512), BF16),
            VM((2, UNITS, width), BF16),
            VM((CORES, 2, PAD, width), BF16),
            VM((CORES, 128, 128), BF16),
            VM((CORES, 8, 128), F32),
            VM((128, 128), F32),
            VM((128, 16), F32),
            VM((16, 128), F32),
            VM((4, 4, ROWS, quarter), BF16),
            VM((4, 4, ROWS, quarter), BF16),
            VM((4, 4, ROWS, quarter), BF16),
            VM((4, 4, ROWS, quarter), BF16),
            VM((4, CORES, PAD, quarter), BF16),
            VM((4, CORES, PAD, quarter), BF16),
            VM((TPS, 128, quarter), BF16),
            VM((TPS, 128, quarter), BF16),
            VM((2, UNITS, width), BF16),
            VM((4, 33, 128, 128), BF16),
            VM((STEPS, 2, ROWS, width), BF16),
            VM((CORES, 128, 128), BF16),
            VM((2, CORES, PAD, width), BF16),
            VM((CORES, 128, 128), BF16),
            VM((CORES, 8, 128), F32),
            VM((128, 128), BF16),
            VM((STEPS, 128, 128), BF16),
            VM((8, 128), F32),
            VM((STEPS, 8, 128), F32),
            VM((CORES, 128, 128), BF16),
            VM((CORES, 128, 128), F32),
            VM((128, 128), F32),
            VM((128, 512), F32),
            dma((4, 4)), dma((4, 4)), dma((4, 4)), dma((4, 4)), dma((4, 8)), dma((4, 8)),
            dma((4,)), dma((4,)),
            dma((2,)), dma((2,)), dma((2,)), dma((6,)), dma((6,)), dma((8,)), dma((8,)),
            dma((4,)), dma((4,)), dma((5, 4)), dma((4, 4)), dma((5,)), dma((4,)),
            dma((4, 4)), dma((4, 4)),
            dma((2, 8)), dma((2, 8)), dma((3, 2)), dma((3, 2)), dma((4, 2)), dma((4, 2)),
            dma((8,)), dma((8,)), dma((8,)), dma((8,)), dma((8,)), dma((8,)),
            dma((8,)), dma((8,)), dma((8,)), dma((8,)),
        ],
        compiler_params=pltpu.CompilerParams(
            collective_id=1, has_side_effects=True, vmem_limit_bytes=58 << 20
        ),
        name="spread",
    )(*operands)


def state_body(inputs, gate, inflow, readout, cum, cum_t, step_t, skip, gain, ent, out, gated):
    low = lax.broadcasted_iota(jnp.int32, (128, 128), 1) < 64
    causal = lax.broadcasted_iota(jnp.int32, (128, 128), 0) >= lax.broadcasted_iota(
        jnp.int32, (128, 128), 1)
    for g in range(2):
        cols = slice(128 * g, 128 * g + 128)
        read = readout[:, cols]
        rw = lax.dot_general(
            read, inflow[:, cols], (((1,), (1,)), ((), ())), preferred_element_type=F32
        )
        square = jnp.zeros((128, 1), F32)
        for p in range(4):
            pair = 4 * g + p
            at = slice(128 * pair, 128 * pair + 128)
            both = inputs[:, at]
            parts = []
            scales = []
            for h in range(2):
                head = 2 * pair + h
                own = cum[:, head:head + 1]
                gap = jnp.where(causal, own - cum_t[head:head + 1, :], 0.0)
                mixing = jnp.where(causal, jnp.exp(gap), 0.0) * rw * step_t[head:head + 1, :]
                parts.append(
                    jnp.dot(mixing.astype(BF16), both, preferred_element_type=F32)
                )
                scales.append(jnp.exp(own))
            intra = jnp.where(low, parts[0], parts[1])
            scale = jnp.where(low, scales[0], scales[1])
            inter = scale * lax.dot_general(
                read, ent[pair], (((1,), (1,)), ((), ())), preferred_element_type=F32
            )
            direct = jnp.where(
                low, skip[:, 2 * pair:2 * pair + 1], skip[:, 2 * pair + 1:2 * pair + 2]
            )
            mixed = intra + inter + direct * both.astype(F32)
            v = gate[:, at].astype(F32)
            value = mixed * (v / (1.0 + jnp.exp(-v)))
            gated[:, 128 * p:128 * p + 128] = value
            square = square + jnp.sum(value * value, axis=1, keepdims=True)
        inv = lax.rsqrt(square / 512.0 + EPSILON)
        wide = slice(512 * g, 512 * g + 512)
        out[:, wide] = (gated[...] * inv * gain[:, wide]).astype(BF16)


def local(
    query_heads, key_heads, value_head_rows, state_input, state_gate, state_inflow,
    state_readout, step_size, log_decay, skip_scale, state_gain, hidden_in, mlp_gain,
    router_weight, expert_ids, slot_index, gate_up, down_proj,
):
    tp = lax.axis_index("tp")
    is_live = slot_index >= 0
    quarter = slot_index // QUARTER
    inside = slot_index - quarter * QUARTER
    near = is_live & (quarter % 2 == tp % 2)
    place = jnp.where(near, expert_ids * (2 * PAD) + (quarter // 2) * PAD + inside, -1)
    home = jnp.where(is_live & (quarter == tp), expert_ids * PAD + inside, -1)
    ints = jnp.concatenate([place, home, expert_ids], axis=1)
    kv_in = jnp.concatenate(
        [jnp.transpose(key_heads, (1, 0, 2)), jnp.transpose(value_head_rows, (1, 0, 2))], axis=0
    )
    heads, state_out, routed_out = spread(
        kv_in, hidden_in, mlp_gain[None], router_weight.T, ints,
        jnp.transpose(gate_up[0], (1, 0, 2)), down_proj[0],
        jnp.transpose(query_heads, (1, 0, 2)).reshape(2, 512, 128),
        state_input, state_gate, state_inflow.reshape(128, 256), state_readout.reshape(128, 256),
        log_decay.T, step_size.T, skip_scale[None], state_gain[None],
    )
    window_out = jnp.transpose(heads.reshape(8, 128, 128), (1, 0, 2))
    return window_out, state_out, routed_out


def solution(mesh):
    both = ("seq", "exp")
    placed = (
        P(both, "tp", None), P(both, "tp", None), P(both, "tp", None),
        P(both, "tp"), P(both, "tp"), P(both, "tp", None), P(both, "tp", None),
        P(both, "tp"), P(both, "tp"), P("tp"), P("tp"), P(both, None), P(), P(),
        P(both, None), P(both, None),
        P("exp", ("seq", "tp"), None, None), P("exp", ("seq", "tp"), None),
    )
    return jax.shard_map(
        local,
        mesh=mesh,
        in_specs=placed,
        out_specs=(P(both, "tp", None), P(both, "tp"), P(both, "tp")),
        check_vma=False,
    )
```

```python
import functools
import math

import jax
import jax.numpy as jnp
from jax import lax
from jax.experimental import pallas as pl
from jax.experimental.pallas import tpu as pltpu
from jax.sharding import PartitionSpec as P

EXPERTS = 8
CAP = 40
STEPS = 8
CORES = 8
TPS = 4
QUARTER = 10
PAD = 16
ROWS = 80
UNITS = 448
HALF = 112
EPSILON = 1e-05
VM = pltpu.VMEM
MESH = pl.DeviceIdType.MESH
F32 = jnp.float32
BF16 = jnp.bfloat16


def rcopy(src, dst, ss, rs, dev):
    return pltpu.make_async_remote_copy(
        src_ref=src, dst_ref=dst, send_sem=ss, recv_sem=rs, device_id=dev, device_id_type=MESH
    )


def guarded(cond, fn):
    if cond is True:
        fn()
    else:
        pl.when(cond)(fn)


def greet(groups):
    barrier = pltpu.get_barrier_semaphore()
    count = 0
    for axis, size, shifts in groups:
        me = lax.axis_index(axis)
        for d in shifts:
            pl.semaphore_signal(
                barrier, inc=1, device_id={axis: lax.rem(me + d, size)}, device_id_type=MESH
            )
            count += 1
    return lambda: pl.semaphore_wait(barrier, count)


def attend_body(s, e, q, kv, out, group):
    row = lax.rem(lax.broadcasted_iota(jnp.int32, (512, 1024), 0), 128)
    col = lax.broadcasted_iota(jnp.int32, (512, 1024), 1)
    place = col // 128
    inside = lax.rem(col, 128)
    far_ok = s >= 4
    near = (place < e) | ((place == e) & (inside <= row)) | ((place > e) & far_ok)
    vrow = lax.broadcasted_iota(jnp.int32, (1024, 128), 0) // 128
    v_ok = (vrow <= e) | far_ok
    last = (
        lax.broadcasted_iota(jnp.int32, (512, 128), 1)
        > lax.rem(lax.broadcasted_iota(jnp.int32, (512, 128), 0), 128)
    ) & far_ok
    scale = 1.0 / math.sqrt(128) * math.log2(math.e)

    def chunk(carried, query, keys, values, mask):
        top, total, acc = carried
        scores = lax.dot_general(
            query, keys, (((1,), (1,)), ((), ())), preferred_element_type=F32
        )
        if mask is not None:
            scores = jnp.where(mask, scores, -1e30)
        new = jnp.maximum(top, jnp.max(scores, axis=1, keepdims=True))
        weights = jnp.exp2((scores - new) * scale)
        if mask is not None:
            weights = jnp.where(mask, weights, 0.0)
        factor = jnp.exp2((top - new) * scale)
        total = total * factor + jnp.sum(weights, axis=1, keepdims=True)
        acc = acc * factor + jnp.dot(
            weights.astype(BF16), values, preferred_element_type=F32
        )
        return new, total, acc

    query = q[group]
    k0 = kv[group, 0:8].reshape(1024, 128)
    v0 = jnp.where(v_ok, kv[2 + group, 0:8].reshape(1024, 128), jnp.zeros((), BF16))
    state = (
        jnp.full((512, 1), -1e30, F32),
        jnp.zeros((512, 1), F32),
        jnp.zeros((512, 128), F32),
    )
    state = chunk(state, query, k0, v0, near)
    vl = jnp.where(far_ok, kv[2 + group, 32], jnp.zeros((), BF16))
    state = chunk(state, query, kv[group, 32], vl, last)

    def more(k, carried):
        keys = kv[group, pl.ds(k * 8, 8)].reshape(1024, 128)
        values = kv[2 + group, pl.ds(k * 8, 8)].reshape(1024, 128)
        return chunk(carried, query, keys, values, None)

    _, total, acc = lax.fori_loop(1, jnp.minimum(s, 3) + 1, more, state)
    out[group] = (acc / total).astype(BF16)


def spread_kernel(
    kv_in, hidden, mlp_gain, router_t, expert_t, slot_t, gu_in, dn_in, q,
    inputs, gate, inflow, readout, decay_t, step_t, skip,
    heads, state_out, routed,
    h_all, h_oth, dn, rows_in, st_in, dec_in, weigh, cum, cum_t,
    tx_f, rx_f, tx_b, rx_b, slots_tx, slots, mine_tx, mine,
    gu, kv, rows, ent, disp, st_rx, dec_rx, t_tx, t_rx, td_tx, td_rx, ent_tx, inner, carry, gated,
    qf_s, qf_r, qb_s, qb_r, o_s, o_r, y_s, y_r,
    l_s, g_s, g_r, n_s, n_r, h_s, h_r,
    z_s, z_r, x_s, x_r, p_s, p_r, f_s, f_r,
    d_s, d_r, rf_s, rf_r, rb_s, rb_r, sa_s, sa_r, da_s, da_r, st_s, st_r, sd_s, sd_r, se_s, se_r,
):
    s = lax.axis_index("seq")
    e = lax.axis_index("exp")
    t = lax.axis_index("tp")
    x = e // 2
    c = lax.rem(e, 2)
    partner = e + 1 - 2 * c
    nxt = lax.rem(s + 1, STEPS)
    prv = lax.rem(s + STEPS - 1, STEPS)
    odd = lax.rem(t, 2)
    to_a = {"tp": t + 1 - 2 * odd}
    to_b = {"tp": lax.rem(t + 3 + 2 * odd, TPS)}
    own = t // 2
    turn = (1 - own, own)
    to_mate = {"tp": lax.rem(t + 2, TPS)}
    all_here = greet(
        (
            ("tp", TPS, range(1, TPS)),
            ("exp", CORES, range(1, CORES)),
            ("seq", STEPS, range(1, STEPS)),
        )
    )
    wide = hidden[...].astype(F32)
    level = lax.rsqrt(jnp.mean(wide * wide, axis=1, keepdims=True) + EPSILON)
    normed = (wide * level * mlp_gain[...]).astype(BF16)
    spot = slot_t[...]
    quarter = sum((spot >= QUARTER * k).astype(jnp.int32) for k in range(1, TPS))
    inside = spot - QUARTER * quarter
    near = (spot >= 0) & ((quarter & 1) == odd)
    place = jnp.where(near, expert_t[...] * (2 * PAD) + (quarter >> 1) * PAD + inside, -1)
    home = jnp.where((spot >= 0) & (quarter == t), expert_t[...] * PAD + inside, -1)
    spots = lax.broadcasted_iota(jnp.int32, (CORES * 2 * PAD, 128), 0)
    picker = ((place[0:1] == spots) | (place[1:2] == spots)).astype(F32).astype(BF16)
    rows_in[...] = jnp.dot(
        picker, normed, preferred_element_type=F32
    ).astype(BF16).reshape(CORES, 2, PAD, -1)
    all_here()
    pending = []

    def send(copy, cond=True):
        guarded(cond, copy.start)
        pending.append((copy, cond))

    def slot_of(k):
        return 32 if k == 4 else k * 8 + e

    def block(k):
        return kv_in if k == 0 else kv.at[:, slot_of(k)]

    def kv_hop(k):
        return rcopy(
            block(k - 1), kv.at[:, slot_of(k)], z_s.at[k - 1], z_r.at[k - 1], {"seq": nxt}
        )

    def kv_across(g, k):
        for dx in range(1, 4):
            tx = lax.rem(x + dx, 4)
            if k == 0:
                cond = tx > x
            elif k == 4:
                cond = (tx < x) & (s >= 4)
            else:
                cond = s >= k
            send(
                rcopy(
                    block(k), kv.at[:, g * 8 + e], x_s.at[k, dx], x_r.at[g, dx],
                    {"exp": 2 * tx + c},
                ),
                cond,
            )
        if k == 0:
            cond = c == 0
        elif k == 4:
            cond = (c == 1) & (s >= 4)
        else:
            cond = s >= k
        send(
            rcopy(block(k), kv.at[:, g * 8 + e], p_s.at[k], p_r.at[g], {"exp": partner}), cond
        )

    def kv_forward(g):
        for dx in range(1, 4):
            sx = lax.rem(x + 4 - dx, 4)
            cond = ((sx < x) | (s >= 4)) if g == 0 else s >= g
            slot = kv.at[:, g * 8 + 2 * sx + c]
            arrived = rcopy(slot, slot, x_s.at[g, dx], x_r.at[g, dx], {"exp": 2 * sx + c})
            onward = rcopy(slot, slot, f_s.at[g, dx], f_r.at[g, dx], {"exp": partner})

            def pass_on(arrived=arrived, onward=onward):
                arrived.wait_recv()
                onward.start()

            guarded(cond, pass_on)
            pending.append((onward, cond))

    def kv_finish(g):
        slot = kv.at[:, g * 8 + partner]
        cond = ((c == 1) | (s >= 4)) if g == 0 else s >= g
        guarded(cond, rcopy(slot, slot, p_s.at[g], p_r.at[g], {"exp": partner}).wait_recv)
        for dx in range(1, 4):
            sx = lax.rem(x + 4 - dx, 4)
            cond = ((sx < x) | (s >= 4)) if g == 0 else s >= g
            slot = kv.at[:, g * 8 + 2 * sx + 1 - c]
            guarded(
                cond, rcopy(slot, slot, f_s.at[g, dx], f_r.at[g, dx], {"exp": partner}).wait_recv
            )

    def kv_arrive(k):
        slot = kv.at[:, slot_of(k)]
        guarded(
            s >= k, rcopy(slot, slot, z_s.at[k - 1], z_r.at[k - 1], {"seq": prv}).wait_recv
        )
        if k < 4:
            send(kv_hop(k + 1), (s >= k) & (s < STEPS - 1))
        kv_across(0 if k == 4 else k, k)

    for i in range(2):
        for d in range(1, CORES):
            to = lax.rem(e + d, CORES)
            send(rcopy(rows_in.at[to, turn[i]], disp.at[i, e], d_s.at[i, d], d_r.at[i, d], {"exp": to}))
        disp[i, pl.ds(e, 1)] = rows_in[pl.ds(e, 1), turn[i]]

    first, second = pl.ds(0, HALF), pl.ds(HALF, HALF)
    third, fourth = pl.ds(2 * HALF, HALF), pl.ds(3 * HALF, HALF)
    send(rcopy(gu_in.at[:, first], gu.at[:, third], g_s.at[0], g_r.at[0], to_a))
    send(rcopy(gu_in.at[:, second], gu.at[:, fourth], g_s.at[1], g_r.at[1], to_b))
    send(kv_hop(1), s < STEPS - 1)
    send(rcopy(dn_in.at[first], dn.at[0, third], n_s.at[0], n_r.at[0], to_a))
    send(rcopy(dn_in.at[second], dn.at[0, fourth], n_s.at[1], n_r.at[1], to_b))
    send(rcopy(dn_in.at[second], dn.at[1, fourth], n_s.at[2], n_r.at[2], to_a))
    send(rcopy(dn_in.at[first], dn.at[1, third], n_s.at[3], n_r.at[3], to_b))
    own_gu = pltpu.make_async_copy(gu_in, gu.at[:, pl.ds(0, 2 * HALF)], l_s.at[0])
    own_dn = pltpu.make_async_copy(dn_in, dn.at[0, pl.ds(0, 2 * HALF)], l_s.at[1])
    own_gu.start()
    own_dn.start()
    exact = lax.Precision.HIGHEST
    low_tri = (
        lax.broadcasted_iota(jnp.int32, (128, 128), 0)
        >= lax.broadcasted_iota(jnp.int32, (128, 128), 1)
    ).astype(F32)
    eye = (
        lax.broadcasted_iota(jnp.int32, (128, 128), 0)
        == lax.broadcasted_iota(jnp.int32, (128, 128), 1)
    ).astype(F32)
    both_last = (((1,), (1,)), ((), ()))
    cum[...] = lax.dot_general(
        low_tri, decay_t[...], both_last, precision=exact, preferred_element_type=F32
    )
    cum_t[...] = lax.dot_general(
        decay_t[...], low_tri, both_last, precision=exact, preferred_element_type=F32
    )
    block_total = cum_t[:, 127:128]
    weight_t = jnp.exp(block_total - cum_t[...]) * step_t[...]
    weight_in = lax.dot_general(
        eye, weight_t, both_last, precision=exact, preferred_element_type=F32
    )
    whole_decay = jnp.broadcast_to(jnp.exp(block_total), (16, 128))
    dec_in[...] = jnp.zeros_like(dec_in)
    for pair in range(8):
        dec_in[pair, 0:2, :] = whole_decay[2 * pair:2 * pair + 2]
        vectors = inflow[:, 128 * (pair // 4):128 * (pair // 4) + 128].astype(F32)
        both = inputs[:, 128 * pair:128 * pair + 128]
        for h in range(2):
            head = 2 * pair + h
            weighted = (weight_in[:, head:head + 1] * vectors).astype(BF16)
            res = lax.dot_general(
                both, weighted, (((0,), (0,)), ((), ())), preferred_element_type=F32
            )
            st_in[pair, 64 * h:64 * h + 64, :] = res[64 * h:64 * h + 64].astype(BF16)
    for d in range(1, CORES):
        to = lax.rem(e + d, CORES)
        send(rcopy(st_in.at[to], st_rx.at[e], sa_s.at[d], sa_r.at[d], {"exp": to}))
        send(rcopy(dec_in.at[to], dec_rx.at[e], da_s.at[d], da_r.at[d], {"exp": to}))
    kv_across(0, 0)
    kv[:, pl.ds(e, 1)] = kv_in[...][:, None]
    st_rx[pl.ds(e, 1)] = st_in[pl.ds(e, 1)]
    dec_rx[pl.ds(e, 1)] = dec_in[pl.ds(e, 1)]
    td_tx[...] = jnp.zeros_like(td_tx)
    h_all[...] = jnp.zeros_like(h_all)
    lane = lax.broadcasted_iota(jnp.int32, (ROWS, CORES * PAD), 1)
    place = (lane // PAD) * QUARTER + lax.rem(lane, PAD)
    fits = lax.rem(lane, PAD) < QUARTER
    pack = (
        (place == lax.broadcasted_iota(jnp.int32, (ROWS, CORES * PAD), 0)) & fits
    ).astype(F32).astype(BF16)

    kv_arrive(1)

    def rows_up(j, i):
        at = rows.at[lax.rem(s + STEPS - j, STEPS), turn[i]]
        return rcopy(at, at, rf_s.at[j, i], rf_r.at[j, i], {"seq": nxt})

    def rows_down(j, i):
        at = rows.at[lax.rem(s + j, STEPS), turn[i]]
        return rcopy(at, at, rb_s.at[j, i], rb_r.at[j, i], {"seq": prv})

    def rows_up_arrived(j, i):
        at = rows.at[lax.rem(s + STEPS - 1 - j, STEPS), turn[i]]
        return rcopy(at, at, rf_s.at[j, i], rf_r.at[j, i], {"seq": prv})

    def rows_down_arrived(j, i):
        at = rows.at[lax.rem(s + 1 + j, STEPS), turn[i]]
        return rcopy(at, at, rb_s.at[j, i], rb_r.at[j, i], {"seq": nxt})

    for i in range(2):
        for d in range(1, CORES):
            frm = lax.rem(e + CORES - d, CORES)
            at = disp.at[i, frm]
            rcopy(at, at, d_s.at[i, d], d_r.at[i, d], {"exp": frm}).wait_recv()
        rows[pl.ds(s, 1), turn[i]] = jnp.dot(
            pack, disp[i].reshape(CORES * PAD, -1), preferred_element_type=F32
        ).astype(BF16)[None]
        send(rows_down(0, i))
        send(rows_up(0, i))
        if i == 0:
            logits = lax.dot_general(
                router_t[...], normed, both_last, preferred_element_type=F32
            )
            gates = 1.0 / (1.0 + jnp.exp(-logits))
            expert = lax.broadcasted_iota(jnp.int32, (EXPERTS, 128), 0)
            chosen = [
                jnp.sum(jnp.where(expert_t[k:k + 1, :] == expert, gates, 0.0), axis=0,
                        keepdims=True)
                for k in range(2)
            ]
            base = lax.broadcasted_iota(jnp.int32, (CORES * PAD, 128), 0)
            weigh[...] = sum(
                jnp.where(home[k:k + 1] == base, chosen[k] / (chosen[0] + chosen[1]), 0.0)
                for k in range(2)
            )
            kv_arrive(2)

    for d in range(1, CORES):
        frm = lax.rem(e + CORES - d, CORES)
        rcopy(st_rx.at[frm], st_rx.at[frm], sa_s.at[d], sa_r.at[d], {"exp": frm}).wait_recv()
        rcopy(dec_rx.at[frm], dec_rx.at[frm], da_s.at[d], da_r.at[d], {"exp": frm}).wait_recv()
    for h in range(2):
        part = slice(64 * h, 64 * h + 64)
        run = jnp.zeros((64, 128), F32)
        whole = jnp.ones((1, 128), F32)
        for k in range(CORES):
            inner[k, part, :] = run
            decay = dec_rx[k, h:h + 1, :]
            run = run * decay + st_rx[k, part, :].astype(F32)
            whole = whole * decay
        t_tx[part, :] = run.astype(BF16)
        td_tx[h:h + 1, :] = whole
    for d in range(1, STEPS):
        to = lax.rem(s + d, STEPS)
        send(rcopy(t_tx, t_rx.at[s], st_s.at[d], st_r.at[d], {"seq": to}), s + d < STEPS)
        send(rcopy(td_tx, td_rx.at[s], sd_s.at[d], sd_r.at[d], {"seq": to}), s + d < STEPS)

    def to_mate_copy(b):
        return rcopy(h_all.at[b, 1 - own], h_oth.at[b], h_s.at[b], h_r.at[b], to_mate)

    def expert_in(b):
        flat = rows[b].reshape(2 * ROWS, -1)
        nt = (((1,), (1,)), ((), ()))
        gated_part = lax.dot_general(flat, gu[0], nt, preferred_element_type=F32)
        up_part = lax.dot_general(flat, gu[1], nt, preferred_element_type=F32)
        units = (gated_part / (1.0 + jnp.exp(-gated_part)) * up_part).astype(BF16)
        h_all[b, 0, :, 0:UNITS] = units[0:ROWS]
        h_all[b, 1, :, 0:UNITS] = units[ROWS:2 * ROWS]
        to_mate_copy(b).start()

    def expert_half(b, which):
        flat = rows[b, which]
        nt = (((1,), (1,)), ((), ()))
        gated_part = lax.dot_general(flat, gu[0], nt, preferred_element_type=F32)
        up_part = lax.dot_general(flat, gu[1], nt, preferred_element_type=F32)
        units = (gated_part / (1.0 + jnp.exp(-gated_part)) * up_part).astype(BF16)
        h_all[b, which, :, 0:UNITS] = units

    def expert_pair(j):
        def one(i, _):
            expert_in(lax.rem(s + STEPS + (2 * i - 1) * (j + 1), STEPS))
            return 0

        lax.fori_loop(0, 2, one, 0)

    def states_in():
        for d in range(1, STEPS):
            frm = lax.rem(s + STEPS - d, STEPS)
            at = t_rx.at[frm]
            guarded(d <= s, rcopy(at, at, st_s.at[d], st_r.at[d], {"seq": frm}).wait_recv)
            at = td_rx.at[frm]
            guarded(d <= s, rcopy(at, at, sd_s.at[d], sd_r.at[d], {"seq": frm}).wait_recv)
        carry[...] = jnp.zeros_like(carry)
        for k in range(STEPS - 1):

            def fold(k=k):
                for h in range(2):
                    part = slice(64 * h, 64 * h + 64)
                    carry[part, :] = carry[part, :] * td_rx[k, h:h + 1, :] + t_rx[
                        k, part, :
                    ].astype(F32)

            pl.when(k < s)(fold)
        for h in range(2):
            part = slice(64 * h, 64 * h + 64)
            moved = carry[part, :]
            for k in range(CORES):
                ent_tx[k, part, :] = (inner[k, part, :] + moved).astype(BF16)
                moved = moved * dec_rx[k, h:h + 1, :]
        for d in range(1, CORES):
            to = lax.rem(e + d, CORES)
            send(rcopy(ent_tx.at[to], ent.at[e], se_s.at[d], se_r.at[d], {"exp": to}))
        ent[pl.ds(e, 1)] = ent_tx[pl.ds(e, 1)]

    def rows_step(j, i):
        rows_down_arrived(j, i).wait_recv()
        if j < 3:
            send(rows_down(j + 1, i))
            rows_up_arrived(j, i).wait_recv()
            if j < 2:
                send(rows_up(j + 1, i))

    rows_step(0, 0)
    kv_arrive(3)
    rows_step(0, 1)
    kv_forward(1)
    own_gu.wait()
    arrive_a = gu.at[:, third]
    arrive_b = gu.at[:, fourth]
    rcopy(arrive_a, arrive_a, g_s.at[0], g_r.at[0], to_a).wait_recv()
    rcopy(arrive_b, arrive_b, g_s.at[1], g_r.at[1], to_b).wait_recv()
    expert_in(s)
    expert_pair(0)
    rows_step(1, 0)
    kv_arrive(4)
    states_in()
    kv_forward(2)
    rows_step(1, 1)
    at = dn.at[0, third]
    rcopy(at, at, n_s.at[0], n_r.at[0], to_a).wait_recv()
    send(rcopy(at, dn.at[1, first], n_s.at[4], n_r.at[4], to_b))
    at = dn.at[0, fourth]
    rcopy(at, at, n_s.at[1], n_r.at[1], to_b).wait_recv()
    send(rcopy(at, dn.at[1, second], n_s.at[5], n_r.at[5], to_a))
    kv_forward(3)
    kv_forward(0)
    expert_pair(1)
    for g in (1, 2, 3, 0):
        kv_finish(g)
    attend_body(s, e, q, kv, heads, 0)
    rows_step(2, 0)
    rows_step(2, 1)
    expert_pair(2)
    attend_body(s, e, q, kv, heads, 1)
    own_dn.wait()
    for n, at, dev in (
        (2, dn.at[1, fourth], to_a),
        (3, dn.at[1, third], to_b),
        (4, dn.at[1, first], to_b),
        (5, dn.at[1, second], to_a),
    ):
        rcopy(at, at, n_s.at[n], n_r.at[n], dev).wait_recv()

    width = dn.shape[-1] // 4

    def columns(stream):
        return slice(width * stream, width * stream + width)

    def mate_arrived(b):
        to_mate_copy(b).wait_recv()

    def partial_of(b, half):
        cols = slice(2 * width * half, 2 * width * (half + 1))
        return jnp.dot(
            h_all[b, own, :, 0:UNITS], dn[0, :, cols], preferred_element_type=F32
        ) + jnp.dot(h_oth[b, :, 0:UNITS], dn[1, :, cols], preferred_element_type=F32)

    def up(stream, j):
        return rcopy(
            tx_f.at[stream, j], rx_f.at[stream, j], qf_s.at[stream, j], qf_r.at[stream, j],
            {"seq": nxt},
        )

    def down(stream, j):
        return rcopy(
            tx_b.at[stream, j], rx_b.at[stream, j], qb_s.at[stream, j], qb_r.at[stream, j],
            {"seq": prv},
        )

    def hop(half, j, rising, value):
        begin = 0 if (half == 0) == rising else 1
        tx, rx, line = (tx_f, rx_f, up) if rising else (tx_b, rx_b, down)
        for i in range(2):
            stream = 2 * half + i
            piece = value[:, columns(i)]
            if j > begin:
                line(stream, j - 1).wait_recv()
                piece = piece + rx[stream, j - 1].astype(F32)
            tx[stream, j] = piece.astype(BF16)
            send(line(stream, j))

    def ahead(d):
        return lax.rem(s + d, STEPS)

    def short_hop(j):
        hop(1, j, True, partial_of(ahead(4 - j), 1))
        hop(0, j, False, partial_of(ahead(4 + j), 0))

    def long_hop(j):
        hop(0, j, True, partial_of(ahead(4 - j), 0))
        hop(1, j, False, partial_of(ahead(4 + j), 1))

    rows_step(3, 0)
    expert_half(ahead(4), 1 - own)
    to_mate_copy(ahead(4)).start()
    mate_arrived(ahead(3))
    mate_arrived(ahead(5))
    short_hop(1)
    rows_step(3, 1)
    expert_half(ahead(4), own)
    for d in (2, 6, 1, 7, 0):
        mate_arrived(ahead(d))
    mate_arrived(ahead(4))
    long_hop(0)
    short_hop(2)
    long_hop(1)
    for d in range(1, CORES):
        frm = lax.rem(e + CORES - d, CORES)
        rcopy(ent.at[frm], ent.at[frm], se_s.at[d], se_r.at[d], {"exp": frm}).wait_recv()

    def recurrence(g):
        state_body(
            inputs, gate, inflow, readout, cum, cum_t, step_t, skip, ent, state_out, gated, g
        )

    recurrence(0)
    long_hop(2)
    short_hop(3)
    recurrence(1)
    long_hop(3)
    finals = [partial_of(s, half) for half in range(2)]

    def slot_copy(stream, d, there):
        return rcopy(
            slots_tx.at[stream, there], slots.at[stream, e], o_s.at[stream, d],
            o_r.at[stream, d], {"exp": there},
        )

    for stream in (0, 2, 1, 3):
        half, i = stream // 2, stream % 2
        up(stream, 3).wait_recv()
        down(stream, 3).wait_recv()
        total = (
            finals[half][:, columns(i)]
            + rx_f[stream, 3].astype(F32)
            + rx_b[stream, 3].astype(F32)
        )
        spaced = lax.dot_general(
            pack, total.astype(BF16), (((0,), (0,)), ((), ())), preferred_element_type=F32
        )
        slots_tx[stream] = spaced.astype(BF16).reshape(CORES, PAD, width)
        for d in range(1, CORES):
            send(slot_copy(stream, d, lax.rem(e + d, CORES)))
        slots[stream, pl.ds(e, 1)] = slots_tx[stream, pl.ds(e, 1)]
    both_first = (((0,), (0,)), ((), ()))
    high = weigh[...].astype(BF16)
    rest = (weigh[...] - high.astype(F32)).astype(BF16)
    for stream in (0, 2, 1, 3):
        for d in range(1, CORES):
            frm = lax.rem(e + CORES - d, CORES)
            at = slots.at[stream, frm]
            rcopy(at, at, o_s.at[stream, d], o_r.at[stream, d], {"exp": frm}).wait_recv()
        at = slots[stream].reshape(CORES * PAD, width)
        mine_tx[stream] = (
            lax.dot_general(high, at, both_first, preferred_element_type=F32)
            + lax.dot_general(rest, at, both_first, preferred_element_type=F32)
        ).astype(BF16)
        send(
            rcopy(mine_tx.at[stream], mine.at[t], y_s.at[stream], y_r.at[t], {"tp": stream}),
            t != stream,
        )
    total = mine_tx[t].astype(F32)
    for d in range(1, TPS):
        frm = lax.rem(t + TPS - d, TPS)
        at = mine.at[frm]
        rcopy(at, at, y_s.at[frm], y_r.at[frm], {"tp": frm}).wait_recv()
        total = total + mine[frm].astype(F32)
    routed[...] = total
    for b in range(STEPS):
        to_mate_copy(b).wait_send()
    for copy, cond in pending:
        guarded(cond, copy.wait_send)


def spread(*operands):
    vm = pl.BlockSpec(memory_space=VM)
    hbm = pl.BlockSpec(memory_space=pl.ANY)
    width = operands[1].shape[-1]
    quarter = width // 4
    dma = pltpu.SemaphoreType.DMA
    return pl.pallas_call(
        spread_kernel,
        out_shape=(
            jax.ShapeDtypeStruct((2, 512, 128), BF16),
            jax.ShapeDtypeStruct((128, 1024), F32),
            jax.ShapeDtypeStruct((128, quarter), F32),
        ),
        in_specs=[vm] * 6 + [hbm] * 2 + [vm] * 8,
        out_specs=(vm,) * 3,
        scratch_shapes=[
            VM((STEPS, 2, ROWS, 512), BF16),
            VM((STEPS, ROWS, 512), BF16),
            VM((2, UNITS, width), BF16),
            VM((CORES, 2, PAD, width), BF16),
            VM((CORES, 128, 128), BF16),
            VM((CORES, 8, 128), F32),
            VM((128, 128), F32),
            VM((128, 16), F32),
            VM((16, 128), F32),
            VM((4, 4, ROWS, quarter), BF16),
            VM((4, 4, ROWS, quarter), BF16),
            VM((4, 4, ROWS, quarter), BF16),
            VM((4, 4, ROWS, quarter), BF16),
            VM((4, CORES, PAD, quarter), BF16),
            VM((4, CORES, PAD, quarter), BF16),
            VM((TPS, 128, quarter), BF16),
            VM((TPS, 128, quarter), BF16),
            VM((2, UNITS, width), BF16),
            VM((4, 33, 128, 128), BF16),
            VM((STEPS, 2, ROWS, width), BF16),
            VM((CORES, 128, 128), BF16),
            VM((2, CORES, PAD, width), BF16),
            VM((CORES, 128, 128), BF16),
            VM((CORES, 8, 128), F32),
            VM((128, 128), BF16),
            VM((STEPS, 128, 128), BF16),
            VM((8, 128), F32),
            VM((STEPS, 8, 128), F32),
            VM((CORES, 128, 128), BF16),
            VM((CORES, 128, 128), F32),
            VM((128, 128), F32),
            VM((128, 512), F32),
            dma((4, 4)), dma((4, 4)), dma((4, 4)), dma((4, 4)), dma((4, 8)), dma((4, 8)),
            dma((4,)), dma((4,)),
            dma((2,)), dma((2,)), dma((2,)), dma((6,)), dma((6,)), dma((8,)), dma((8,)),
            dma((4,)), dma((4,)), dma((5, 4)), dma((4, 4)), dma((5,)), dma((4,)),
            dma((4, 4)), dma((4, 4)),
            dma((2, 8)), dma((2, 8)), dma((3, 2)), dma((3, 2)), dma((4, 2)), dma((4, 2)),
            dma((8,)), dma((8,)), dma((8,)), dma((8,)), dma((8,)), dma((8,)),
            dma((8,)), dma((8,)), dma((8,)), dma((8,)),
        ],
        compiler_params=pltpu.CompilerParams(
            collective_id=1, has_side_effects=True, vmem_limit_bytes=58 << 20
        ),
        name="spread",
    )(*operands)


def state_body(inputs, gate, inflow, readout, cum, cum_t, step_t, skip, ent, out, gated, g):
    low = lax.broadcasted_iota(jnp.int32, (128, 128), 1) < 64
    causal = lax.broadcasted_iota(jnp.int32, (128, 128), 0) >= lax.broadcasted_iota(
        jnp.int32, (128, 128), 1)
    cols = slice(128 * g, 128 * g + 128)
    read = readout[:, cols]
    rw = lax.dot_general(
        read, inflow[:, cols], (((1,), (1,)), ((), ())), preferred_element_type=F32
    )
    square = jnp.zeros((128, 1), F32)
    for p in range(4):
        pair = 4 * g + p
        at = slice(128 * pair, 128 * pair + 128)
        both = inputs[:, at]
        parts = []
        scales = []
        for h in range(2):
            head = 2 * pair + h
            own = cum[:, head:head + 1]
            gap = jnp.where(causal, own - cum_t[head:head + 1, :], 0.0)
            mixing = jnp.where(causal, jnp.exp(gap), 0.0) * rw * step_t[head:head + 1, :]
            parts.append(
                jnp.dot(mixing.astype(BF16), both, preferred_element_type=F32)
            )
            scales.append(jnp.exp(own))
        intra = jnp.where(low, parts[0], parts[1])
        scale = jnp.where(low, scales[0], scales[1])
        inter = scale * lax.dot_general(
            read, ent[pair], (((1,), (1,)), ((), ())), preferred_element_type=F32
        )
        direct = jnp.where(
            low, skip[:, 2 * pair:2 * pair + 1], skip[:, 2 * pair + 1:2 * pair + 2]
        )
        mixed = intra + inter + direct * both.astype(F32)
        v = gate[:, at].astype(F32)
        value = mixed * (v / (1.0 + jnp.exp(-v)))
        gated[:, 128 * p:128 * p + 128] = value
        square = square + jnp.sum(value * value, axis=1, keepdims=True)
    inv = lax.rsqrt(square / 512.0 + EPSILON)
    wide = slice(512 * g, 512 * g + 512)
    out[:, wide] = gated[...] * inv


def local(
    query_heads, key_heads, value_head_rows, state_input, state_gate, state_inflow,
    state_readout, step_size, log_decay, skip_scale, state_gain, hidden_in, mlp_gain,
    router_weight, expert_ids, slot_index, gate_up, down_proj,
):
    kv_in = jnp.concatenate(
        [jnp.transpose(key_heads, (1, 0, 2)), jnp.transpose(value_head_rows, (1, 0, 2))], axis=0
    )
    heads, states, total = spread(
        kv_in, hidden_in, mlp_gain[None], router_weight.T, expert_ids.T, slot_index.T,
        jnp.transpose(gate_up[0], (1, 0, 2)), down_proj[0],
        jnp.transpose(query_heads, (1, 0, 2)).reshape(2, 512, 128),
        state_input, state_gate, state_inflow.reshape(128, 256), state_readout.reshape(128, 256),
        log_decay.T, step_size.T, skip_scale[None],
    )
    window_out = jnp.transpose(heads.reshape(8, 128, 128), (1, 0, 2))
    return window_out, (states * state_gain).astype(BF16), total.astype(BF16)


def solution(mesh):
    both = ("seq", "exp")
    placed = (
        P(both, "tp", None), P(both, "tp", None), P(both, "tp", None),
        P(both, "tp"), P(both, "tp"), P(both, "tp", None), P(both, "tp", None),
        P(both, "tp"), P(both, "tp"), P("tp"), P("tp"), P(both, None), P(), P(),
        P(both, None), P(both, None),
        P("exp", ("seq", "tp"), None, None), P("exp", ("seq", "tp"), None),
    )
    return jax.shard_map(
        local,
        mesh=mesh,
        in_specs=placed,
        out_specs=(P(both, "tp", None), P(both, "tp"), P(both, "tp")),
        check_vma=False,
    )
```

```python
import functools
import math

import jax
import jax.numpy as jnp
from jax import lax
from jax.experimental import pallas as pl
from jax.experimental.pallas import tpu as pltpu
from jax.sharding import PartitionSpec as P

EXPERTS = 8
CAP = 40
STEPS = 8
CORES = 8
TPS = 4
QUARTER = 10
PAD = 16
ROWS = 80
UNITS = 448
HALF = 112
EPSILON = 1e-05
VM = pltpu.VMEM
MESH = pl.DeviceIdType.MESH
F32 = jnp.float32
BF16 = jnp.bfloat16


def rcopy(src, dst, ss, rs, dev):
    return pltpu.make_async_remote_copy(
        src_ref=src, dst_ref=dst, send_sem=ss, recv_sem=rs, device_id=dev, device_id_type=MESH
    )


def guarded(cond, fn):
    if cond is True:
        fn()
    else:
        pl.when(cond)(fn)


def greet(groups):
    barrier = pltpu.get_barrier_semaphore()
    count = 0
    for axis, size, shifts in groups:
        me = lax.axis_index(axis)
        for d in shifts:
            pl.semaphore_signal(
                barrier, inc=1, device_id={axis: lax.rem(me + d, size)}, device_id_type=MESH
            )
            count += 1
    return lambda: pl.semaphore_wait(barrier, count)


def attend_body(s, e, q, kv, out, group):
    row = lax.rem(lax.broadcasted_iota(jnp.int32, (512, 1024), 0), 128)
    col = lax.broadcasted_iota(jnp.int32, (512, 1024), 1)
    place = col // 128
    inside = lax.rem(col, 128)
    far_ok = s >= 4
    near = (place < e) | ((place == e) & (inside <= row)) | ((place > e) & far_ok)
    vrow = lax.broadcasted_iota(jnp.int32, (1024, 128), 0) // 128
    v_ok = (vrow <= e) | far_ok
    last = (
        lax.broadcasted_iota(jnp.int32, (512, 128), 1)
        > lax.rem(lax.broadcasted_iota(jnp.int32, (512, 128), 0), 128)
    ) & far_ok
    scale = 1.0 / math.sqrt(128) * math.log2(math.e)

    def chunk(carried, query, keys, values, mask):
        top, total, acc = carried
        scores = lax.dot_general(
            query, keys, (((1,), (1,)), ((), ())), preferred_element_type=F32
        )
        if mask is not None:
            scores = jnp.where(mask, scores, -1e30)
        new = jnp.maximum(top, jnp.max(scores, axis=1, keepdims=True))
        weights = jnp.exp2((scores - new) * scale)
        if mask is not None:
            weights = jnp.where(mask, weights, 0.0)
        factor = jnp.exp2((top - new) * scale)
        total = total * factor + jnp.sum(weights, axis=1, keepdims=True)
        acc = acc * factor + jnp.dot(
            weights.astype(BF16), values, preferred_element_type=F32
        )
        return new, total, acc

    query = jnp.concatenate([q[:, 4 * group + k, :] for k in range(4)], axis=0)
    k0 = kv[group, 0:8].reshape(1024, 128)
    v0 = jnp.where(v_ok, kv[2 + group, 0:8].reshape(1024, 128), jnp.zeros((), BF16))
    state = (
        jnp.full((512, 1), -1e30, F32),
        jnp.zeros((512, 1), F32),
        jnp.zeros((512, 128), F32),
    )
    state = chunk(state, query, k0, v0, near)
    vl = jnp.where(far_ok, kv[2 + group, 32], jnp.zeros((), BF16))
    state = chunk(state, query, kv[group, 32], vl, last)

    def more(k, carried):
        keys = kv[group, pl.ds(k * 8, 8)].reshape(1024, 128)
        values = kv[2 + group, pl.ds(k * 8, 8)].reshape(1024, 128)
        return chunk(carried, query, keys, values, None)

    _, total, acc = lax.fori_loop(1, jnp.minimum(s, 3) + 1, more, state)
    out[group] = (acc / total).astype(BF16)


def spread_kernel(
    kv_in, hidden, mlp_gain, router_t, expert_t, slot_t, gu_in, dn_in, q,
    inputs, gate, inflow, readout, decay_t, step_t, skip,
    heads, state_out, routed,
    h_all, h_oth, dn, rows_in, st_in, dec_in, weigh, cum, cum_t,
    tx_f, rx_f, tx_b, rx_b, slots_tx, slots, mine_tx, mine,
    gu, kv, rows, ent, disp, st_rx, dec_rx, t_tx, t_rx, td_tx, td_rx, ent_tx, inner, carry, gated,
    qf_s, qf_r, qb_s, qb_r, o_s, o_r, y_s, y_r,
    l_s, g_s, g_r, n_s, n_r, h_s, h_r,
    z_s, z_r, x_s, x_r, p_s, p_r, f_s, f_r,
    d_s, d_r, rf_s, rf_r, rb_s, rb_r, sa_s, sa_r, da_s, da_r, st_s, st_r, sd_s, sd_r, se_s, se_r,
):
    s = lax.axis_index("seq")
    e = lax.axis_index("exp")
    t = lax.axis_index("tp")
    x = e // 2
    c = lax.rem(e, 2)
    partner = e + 1 - 2 * c
    nxt = lax.rem(s + 1, STEPS)
    prv = lax.rem(s + STEPS - 1, STEPS)
    odd = lax.rem(t, 2)
    to_a = {"tp": t + 1 - 2 * odd}
    to_b = {"tp": lax.rem(t + 3 + 2 * odd, TPS)}
    own = t // 2
    turn = (1 - own, own)
    to_mate = {"tp": lax.rem(t + 2, TPS)}
    all_here = greet(
        (
            ("tp", TPS, range(1, TPS)),
            ("exp", CORES, range(1, CORES)),
            ("seq", STEPS, range(1, STEPS)),
        )
    )
    wide = hidden[...].astype(F32)
    level = lax.rsqrt(jnp.mean(wide * wide, axis=1, keepdims=True) + EPSILON)
    normed = (wide * level * mlp_gain[...]).astype(BF16)
    spot = slot_t[...]
    quarter = sum((spot >= QUARTER * k).astype(jnp.int32) for k in range(1, TPS))
    inside = spot - QUARTER * quarter
    near = (spot >= 0) & ((quarter & 1) == odd)
    place = jnp.where(near, expert_t[...] * (2 * PAD) + (quarter >> 1) * PAD + inside, -1)
    home = jnp.where((spot >= 0) & (quarter == t), expert_t[...] * PAD + inside, -1)
    spots = lax.broadcasted_iota(jnp.int32, (CORES * 2 * PAD, 128), 0)
    picker = ((place[0:1] == spots) | (place[1:2] == spots)).astype(F32).astype(BF16)
    rows_in[...] = jnp.dot(
        picker, normed, preferred_element_type=F32
    ).astype(BF16).reshape(CORES, 2, PAD, -1)
    all_here()
    pending = []

    def send(copy, cond=True):
        guarded(cond, copy.start)
        pending.append((copy, cond))

    def slot_of(k):
        return 32 if k == 4 else k * 8 + e

    def block(k):
        return kv_in if k == 0 else kv.at[:, slot_of(k)]

    def kv_hop(k):
        return rcopy(
            block(k - 1), kv.at[:, slot_of(k)], z_s.at[k - 1], z_r.at[k - 1], {"seq": nxt}
        )

    def kv_across(g, k):
        for dx in range(1, 4):
            tx = lax.rem(x + dx, 4)
            if k == 0:
                cond = tx > x
            elif k == 4:
                cond = (tx < x) & (s >= 4)
            else:
                cond = s >= k
            send(
                rcopy(
                    block(k), kv.at[:, g * 8 + e], x_s.at[k, dx], x_r.at[g, dx],
                    {"exp": 2 * tx + c},
                ),
                cond,
            )
        if k == 0:
            cond = c == 0
        elif k == 4:
            cond = (c == 1) & (s >= 4)
        else:
            cond = s >= k
        send(
            rcopy(block(k), kv.at[:, g * 8 + e], p_s.at[k], p_r.at[g], {"exp": partner}), cond
        )

    def kv_forward(g):
        for dx in range(1, 4):
            sx = lax.rem(x + 4 - dx, 4)
            cond = ((sx < x) | (s >= 4)) if g == 0 else s >= g
            slot = kv.at[:, g * 8 + 2 * sx + c]
            arrived = rcopy(slot, slot, x_s.at[g, dx], x_r.at[g, dx], {"exp": 2 * sx + c})
            onward = rcopy(slot, slot, f_s.at[g, dx], f_r.at[g, dx], {"exp": partner})

            def pass_on(arrived=arrived, onward=onward):
                arrived.wait_recv()
                onward.start()

            guarded(cond, pass_on)
            pending.append((onward, cond))

    def kv_finish(g):
        slot = kv.at[:, g * 8 + partner]
        cond = ((c == 1) | (s >= 4)) if g == 0 else s >= g
        guarded(cond, rcopy(slot, slot, p_s.at[g], p_r.at[g], {"exp": partner}).wait_recv)
        for dx in range(1, 4):
            sx = lax.rem(x + 4 - dx, 4)
            cond = ((sx < x) | (s >= 4)) if g == 0 else s >= g
            slot = kv.at[:, g * 8 + 2 * sx + 1 - c]
            guarded(
                cond, rcopy(slot, slot, f_s.at[g, dx], f_r.at[g, dx], {"exp": partner}).wait_recv
            )

    def kv_arrive(k):
        slot = kv.at[:, slot_of(k)]
        guarded(
            s >= k, rcopy(slot, slot, z_s.at[k - 1], z_r.at[k - 1], {"seq": prv}).wait_recv
        )
        if k < 4:
            send(kv_hop(k + 1), (s >= k) & (s < STEPS - 1))
        kv_across(0 if k == 4 else k, k)

    for i in range(2):
        for d in range(1, CORES):
            to = lax.rem(e + d, CORES)
            send(rcopy(rows_in.at[to, turn[i]], disp.at[i, e], d_s.at[i, d], d_r.at[i, d], {"exp": to}))
        disp[i, pl.ds(e, 1)] = rows_in[pl.ds(e, 1), turn[i]]

    first, second = pl.ds(0, HALF), pl.ds(HALF, HALF)
    third, fourth = pl.ds(2 * HALF, HALF), pl.ds(3 * HALF, HALF)
    send(rcopy(gu_in.at[:, first], gu.at[:, third], g_s.at[0], g_r.at[0], to_a))
    send(rcopy(gu_in.at[:, second], gu.at[:, fourth], g_s.at[1], g_r.at[1], to_b))
    send(kv_hop(1), s < STEPS - 1)
    send(rcopy(dn_in.at[first], dn.at[0, third], n_s.at[0], n_r.at[0], to_a))
    send(rcopy(dn_in.at[second], dn.at[0, fourth], n_s.at[1], n_r.at[1], to_b))
    send(rcopy(dn_in.at[second], dn.at[1, fourth], n_s.at[2], n_r.at[2], to_a))
    send(rcopy(dn_in.at[first], dn.at[1, third], n_s.at[3], n_r.at[3], to_b))
    own_gu = pltpu.make_async_copy(gu_in, gu.at[:, pl.ds(0, 2 * HALF)], l_s.at[0])
    own_dn = pltpu.make_async_copy(dn_in, dn.at[0, pl.ds(0, 2 * HALF)], l_s.at[1])
    own_gu.start()
    own_dn.start()
    exact = lax.Precision.HIGHEST
    low_tri = (
        lax.broadcasted_iota(jnp.int32, (128, 128), 0)
        >= lax.broadcasted_iota(jnp.int32, (128, 128), 1)
    ).astype(F32)
    eye = (
        lax.broadcasted_iota(jnp.int32, (128, 128), 0)
        == lax.broadcasted_iota(jnp.int32, (128, 128), 1)
    ).astype(F32)
    both_last = (((1,), (1,)), ((), ()))
    cum[...] = lax.dot_general(
        low_tri, decay_t[...], both_last, precision=exact, preferred_element_type=F32
    )
    cum_t[...] = lax.dot_general(
        decay_t[...], low_tri, both_last, precision=exact, preferred_element_type=F32
    )
    block_total = cum_t[:, 127:128]
    weight_t = jnp.exp(block_total - cum_t[...]) * step_t[...]
    weight_in = lax.dot_general(
        eye, weight_t, both_last, precision=exact, preferred_element_type=F32
    )
    whole_decay = jnp.broadcast_to(jnp.exp(block_total), (16, 128))
    dec_in[...] = jnp.zeros_like(dec_in)
    for pair in range(8):
        dec_in[pair, 0:2, :] = whole_decay[2 * pair:2 * pair + 2]
        vectors = inflow[:, pair // 4, :].astype(F32)
        both = inputs[:, 128 * pair:128 * pair + 128]
        for h in range(2):
            head = 2 * pair + h
            weighted = (weight_in[:, head:head + 1] * vectors).astype(BF16)
            res = lax.dot_general(
                both, weighted, (((0,), (0,)), ((), ())), preferred_element_type=F32
            )
            st_in[pair, 64 * h:64 * h + 64, :] = res[64 * h:64 * h + 64].astype(BF16)
    for d in range(1, CORES):
        to = lax.rem(e + d, CORES)
        send(rcopy(st_in.at[to], st_rx.at[e], sa_s.at[d], sa_r.at[d], {"exp": to}))
        send(rcopy(dec_in.at[to], dec_rx.at[e], da_s.at[d], da_r.at[d], {"exp": to}))
    kv_across(0, 0)
    kv[:, pl.ds(e, 1)] = kv_in[...][:, None]
    st_rx[pl.ds(e, 1)] = st_in[pl.ds(e, 1)]
    dec_rx[pl.ds(e, 1)] = dec_in[pl.ds(e, 1)]
    td_tx[...] = jnp.zeros_like(td_tx)
    h_all[...] = jnp.zeros_like(h_all)
    lane = lax.broadcasted_iota(jnp.int32, (ROWS, CORES * PAD), 1)
    place = (lane // PAD) * QUARTER + lax.rem(lane, PAD)
    fits = lax.rem(lane, PAD) < QUARTER
    pack = (
        (place == lax.broadcasted_iota(jnp.int32, (ROWS, CORES * PAD), 0)) & fits
    ).astype(F32).astype(BF16)

    kv_arrive(1)

    def rows_up(j, i):
        at = rows.at[lax.rem(s + STEPS - j, STEPS), turn[i]]
        return rcopy(at, at, rf_s.at[j, i], rf_r.at[j, i], {"seq": nxt})

    def rows_down(j, i):
        at = rows.at[lax.rem(s + j, STEPS), turn[i]]
        return rcopy(at, at, rb_s.at[j, i], rb_r.at[j, i], {"seq": prv})

    def rows_up_arrived(j, i):
        at = rows.at[lax.rem(s + STEPS - 1 - j, STEPS), turn[i]]
        return rcopy(at, at, rf_s.at[j, i], rf_r.at[j, i], {"seq": prv})

    def rows_down_arrived(j, i):
        at = rows.at[lax.rem(s + 1 + j, STEPS), turn[i]]
        return rcopy(at, at, rb_s.at[j, i], rb_r.at[j, i], {"seq": nxt})

    for i in range(2):
        for d in range(1, CORES):
            frm = lax.rem(e + CORES - d, CORES)
            at = disp.at[i, frm]
            rcopy(at, at, d_s.at[i, d], d_r.at[i, d], {"exp": frm}).wait_recv()
        rows[pl.ds(s, 1), turn[i]] = jnp.dot(
            pack, disp[i].reshape(CORES * PAD, -1), preferred_element_type=F32
        ).astype(BF16)[None]
        send(rows_down(0, i))
        send(rows_up(0, i))
        if i == 0:
            logits = lax.dot_general(
                router_t[...], normed, both_last, preferred_element_type=F32
            )
            gates = 1.0 / (1.0 + jnp.exp(-logits))
            expert = lax.broadcasted_iota(jnp.int32, (EXPERTS, 128), 0)
            chosen = [
                jnp.sum(jnp.where(expert_t[k:k + 1, :] == expert, gates, 0.0), axis=0,
                        keepdims=True)
                for k in range(2)
            ]
            base = lax.broadcasted_iota(jnp.int32, (CORES * PAD, 128), 0)
            weigh[...] = sum(
                jnp.where(home[k:k + 1] == base, chosen[k] / (chosen[0] + chosen[1]), 0.0)
                for k in range(2)
            )
            kv_arrive(2)

    for d in range(1, CORES):
        frm = lax.rem(e + CORES - d, CORES)
        rcopy(st_rx.at[frm], st_rx.at[frm], sa_s.at[d], sa_r.at[d], {"exp": frm}).wait_recv()
        rcopy(dec_rx.at[frm], dec_rx.at[frm], da_s.at[d], da_r.at[d], {"exp": frm}).wait_recv()
    for h in range(2):
        part = slice(64 * h, 64 * h + 64)
        run = jnp.zeros((64, 128), F32)
        whole = jnp.ones((1, 128), F32)
        for k in range(CORES):
            inner[k, part, :] = run
            decay = dec_rx[k, h:h + 1, :]
            run = run * decay + st_rx[k, part, :].astype(F32)
            whole = whole * decay
        t_tx[part, :] = run.astype(BF16)
        td_tx[h:h + 1, :] = whole
    for d in range(1, STEPS):
        to = lax.rem(s + d, STEPS)
        send(rcopy(t_tx, t_rx.at[s], st_s.at[d], st_r.at[d], {"seq": to}), s + d < STEPS)
        send(rcopy(td_tx, td_rx.at[s], sd_s.at[d], sd_r.at[d], {"seq": to}), s + d < STEPS)

    def to_mate_copy(b):
        return rcopy(h_all.at[b, 1 - own], h_oth.at[b], h_s.at[b], h_r.at[b], to_mate)

    def expert_in(b):
        flat = rows[b].reshape(2 * ROWS, -1)
        nt = (((1,), (1,)), ((), ()))
        gated_part = lax.dot_general(flat, gu[0], nt, preferred_element_type=F32)
        up_part = lax.dot_general(flat, gu[1], nt, preferred_element_type=F32)
        units = (gated_part / (1.0 + jnp.exp(-gated_part)) * up_part).astype(BF16)
        h_all[b, 0, :, 0:UNITS] = units[0:ROWS]
        h_all[b, 1, :, 0:UNITS] = units[ROWS:2 * ROWS]
        to_mate_copy(b).start()

    def expert_half(b, which):
        flat = rows[b, which]
        nt = (((1,), (1,)), ((), ()))
        gated_part = lax.dot_general(flat, gu[0], nt, preferred_element_type=F32)
        up_part = lax.dot_general(flat, gu[1], nt, preferred_element_type=F32)
        units = (gated_part / (1.0 + jnp.exp(-gated_part)) * up_part).astype(BF16)
        h_all[b, which, :, 0:UNITS] = units

    def expert_pair(j):
        def one(i, _):
            expert_in(lax.rem(s + STEPS + (2 * i - 1) * (j + 1), STEPS))
            return 0

        lax.fori_loop(0, 2, one, 0)

    def states_in():
        for d in range(1, STEPS):
            frm = lax.rem(s + STEPS - d, STEPS)
            at = t_rx.at[frm]
            guarded(d <= s, rcopy(at, at, st_s.at[d], st_r.at[d], {"seq": frm}).wait_recv)
            at = td_rx.at[frm]
            guarded(d <= s, rcopy(at, at, sd_s.at[d], sd_r.at[d], {"seq": frm}).wait_recv)
        carry[...] = jnp.zeros_like(carry)
        for k in range(STEPS - 1):

            def fold(k=k):
                for h in range(2):
                    part = slice(64 * h, 64 * h + 64)
                    carry[part, :] = carry[part, :] * td_rx[k, h:h + 1, :] + t_rx[
                        k, part, :
                    ].astype(F32)

            pl.when(k < s)(fold)
        for h in range(2):
            part = slice(64 * h, 64 * h + 64)
            moved = carry[part, :]
            for k in range(CORES):
                ent_tx[k, part, :] = (inner[k, part, :] + moved).astype(BF16)
                moved = moved * dec_rx[k, h:h + 1, :]
        for d in range(1, CORES):
            to = lax.rem(e + d, CORES)
            send(rcopy(ent_tx.at[to], ent.at[e], se_s.at[d], se_r.at[d], {"exp": to}))
        ent[pl.ds(e, 1)] = ent_tx[pl.ds(e, 1)]

    def rows_step(j, i):
        rows_down_arrived(j, i).wait_recv()
        if j < 3:
            send(rows_down(j + 1, i))
            rows_up_arrived(j, i).wait_recv()
            if j < 2:
                send(rows_up(j + 1, i))

    rows_step(0, 0)
    kv_arrive(3)
    rows_step(0, 1)
    kv_forward(1)
    own_gu.wait()
    arrive_a = gu.at[:, third]
    arrive_b = gu.at[:, fourth]
    rcopy(arrive_a, arrive_a, g_s.at[0], g_r.at[0], to_a).wait_recv()
    rcopy(arrive_b, arrive_b, g_s.at[1], g_r.at[1], to_b).wait_recv()
    expert_in(s)
    expert_pair(0)
    rows_step(1, 0)
    kv_arrive(4)
    states_in()
    kv_forward(2)
    rows_step(1, 1)
    at = dn.at[0, third]
    rcopy(at, at, n_s.at[0], n_r.at[0], to_a).wait_recv()
    send(rcopy(at, dn.at[1, first], n_s.at[4], n_r.at[4], to_b))
    at = dn.at[0, fourth]
    rcopy(at, at, n_s.at[1], n_r.at[1], to_b).wait_recv()
    send(rcopy(at, dn.at[1, second], n_s.at[5], n_r.at[5], to_a))
    kv_forward(3)
    kv_forward(0)
    expert_pair(1)
    for g in (1, 2, 3, 0):
        kv_finish(g)
    attend_body(s, e, q, kv, heads, 0)
    rows_step(2, 0)
    rows_step(2, 1)
    expert_pair(2)
    attend_body(s, e, q, kv, heads, 1)
    own_dn.wait()
    for n, at, dev in (
        (2, dn.at[1, fourth], to_a),
        (3, dn.at[1, third], to_b),
        (4, dn.at[1, first], to_b),
        (5, dn.at[1, second], to_a),
    ):
        rcopy(at, at, n_s.at[n], n_r.at[n], dev).wait_recv()

    width = dn.shape[-1] // 4

    def columns(stream):
        return slice(width * stream, width * stream + width)

    def mate_arrived(b):
        to_mate_copy(b).wait_recv()

    def partial_of(b, half):
        cols = slice(2 * width * half, 2 * width * (half + 1))
        return jnp.dot(
            h_all[b, own, :, 0:UNITS], dn[0, :, cols], preferred_element_type=F32
        ) + jnp.dot(h_oth[b, :, 0:UNITS], dn[1, :, cols], preferred_element_type=F32)

    def up(stream, j):
        return rcopy(
            tx_f.at[stream, j], rx_f.at[stream, j], qf_s.at[stream, j], qf_r.at[stream, j],
            {"seq": nxt},
        )

    def down(stream, j):
        return rcopy(
            tx_b.at[stream, j], rx_b.at[stream, j], qb_s.at[stream, j], qb_r.at[stream, j],
            {"seq": prv},
        )

    def hop(half, j, rising, value, i):
        begin = 0 if (half == 0) == rising else 1
        tx, rx, line = (tx_f, rx_f, up) if rising else (tx_b, rx_b, down)
        stream = 2 * half + i
        piece = value[:, columns(i)]
        if j > begin:
            line(stream, j - 1).wait_recv()
            piece = piece + rx[stream, j - 1].astype(F32)
        tx[stream, j] = piece.astype(BF16)
        send(line(stream, j))

    def ahead(d):
        return lax.rem(s + d, STEPS)

    def short_hop(j):
        rise, fall = partial_of(ahead(4 - j), 1), partial_of(ahead(4 + j), 0)
        for i in range(2):
            hop(1, j, True, rise, i)
            hop(0, j, False, fall, i)

    def long_hop(j):
        rise, fall = partial_of(ahead(4 - j), 0), partial_of(ahead(4 + j), 1)
        for i in range(2):
            hop(0, j, True, rise, i)
            hop(1, j, False, fall, i)

    rows_step(3, 0)
    expert_half(ahead(4), 1 - own)
    to_mate_copy(ahead(4)).start()
    mate_arrived(ahead(3))
    mate_arrived(ahead(5))
    short_hop(1)
    rows_step(3, 1)
    expert_half(ahead(4), own)
    for d in (2, 6, 1, 7, 0):
        mate_arrived(ahead(d))
    mate_arrived(ahead(4))
    long_hop(0)
    short_hop(2)
    long_hop(1)
    for d in range(1, CORES):
        frm = lax.rem(e + CORES - d, CORES)
        rcopy(ent.at[frm], ent.at[frm], se_s.at[d], se_r.at[d], {"exp": frm}).wait_recv()

    def recurrence(g):
        state_body(
            inputs, gate, inflow, readout, cum, cum_t, step_t, skip, ent, state_out, gated, g
        )

    recurrence(0)
    long_hop(2)
    short_hop(3)
    recurrence(1)
    long_hop(3)
    finals = [partial_of(s, half) for half in range(2)]

    def slot_copy(stream, d, there):
        return rcopy(
            slots_tx.at[stream, there], slots.at[stream, e], o_s.at[stream, d],
            o_r.at[stream, d], {"exp": there},
        )

    for stream in (0, 2, 1, 3):
        half, i = stream // 2, stream % 2
        up(stream, 3).wait_recv()
        down(stream, 3).wait_recv()
        total = (
            finals[half][:, columns(i)]
            + rx_f[stream, 3].astype(F32)
            + rx_b[stream, 3].astype(F32)
        )
        spaced = lax.dot_general(
            pack, total.astype(BF16), (((0,), (0,)), ((), ())), preferred_element_type=F32
        )
        slots_tx[stream] = spaced.astype(BF16).reshape(CORES, PAD, width)
        for d in range(1, CORES):
            send(slot_copy(stream, d, lax.rem(e + d, CORES)))
        slots[stream, pl.ds(e, 1)] = slots_tx[stream, pl.ds(e, 1)]
    both_first = (((0,), (0,)), ((), ()))
    high = weigh[...].astype(BF16)
    rest = (weigh[...] - high.astype(F32)).astype(BF16)
    for stream in (0, 2, 1, 3):
        for d in range(1, CORES):
            frm = lax.rem(e + CORES - d, CORES)
            at = slots.at[stream, frm]
            rcopy(at, at, o_s.at[stream, d], o_r.at[stream, d], {"exp": frm}).wait_recv()
        at = slots[stream].reshape(CORES * PAD, width)
        mine_tx[stream] = (
            lax.dot_general(high, at, both_first, preferred_element_type=F32)
            + lax.dot_general(rest, at, both_first, preferred_element_type=F32)
        ).astype(BF16)
        send(
            rcopy(mine_tx.at[stream], mine.at[t], y_s.at[stream], y_r.at[t], {"tp": stream}),
            t != stream,
        )
    total = mine_tx[t].astype(F32)
    for d in range(1, TPS):
        frm = lax.rem(t + TPS - d, TPS)
        at = mine.at[frm]
        rcopy(at, at, y_s.at[frm], y_r.at[frm], {"tp": frm}).wait_recv()
        total = total + mine[frm].astype(F32)
    routed[...] = total
    for b in range(STEPS):
        to_mate_copy(b).wait_send()
    for copy, cond in pending:
        guarded(cond, copy.wait_send)


def spread(*operands):
    vm = pl.BlockSpec(memory_space=VM)
    hbm = pl.BlockSpec(memory_space=pl.ANY)
    width = operands[1].shape[-1]
    quarter = width // 4
    dma = pltpu.SemaphoreType.DMA
    return pl.pallas_call(
        spread_kernel,
        out_shape=(
            jax.ShapeDtypeStruct((2, 512, 128), BF16),
            jax.ShapeDtypeStruct((128, 1024), F32),
            jax.ShapeDtypeStruct((128, quarter), F32),
        ),
        in_specs=[vm] * 6 + [hbm] * 2 + [vm] * 8,
        out_specs=(vm,) * 3,
        scratch_shapes=[
            VM((STEPS, 2, ROWS, 512), BF16),
            VM((STEPS, ROWS, 512), BF16),
            VM((2, UNITS, width), BF16),
            VM((CORES, 2, PAD, width), BF16),
            VM((CORES, 128, 128), BF16),
            VM((CORES, 8, 128), F32),
            VM((128, 128), F32),
            VM((128, 16), F32),
            VM((16, 128), F32),
            VM((4, 4, ROWS, quarter), BF16),
            VM((4, 4, ROWS, quarter), BF16),
            VM((4, 4, ROWS, quarter), BF16),
            VM((4, 4, ROWS, quarter), BF16),
            VM((4, CORES, PAD, quarter), BF16),
            VM((4, CORES, PAD, quarter), BF16),
            VM((TPS, 128, quarter), BF16),
            VM((TPS, 128, quarter), BF16),
            VM((2, UNITS, width), BF16),
            VM((4, 33, 128, 128), BF16),
            VM((STEPS, 2, ROWS, width), BF16),
            VM((CORES, 128, 128), BF16),
            VM((2, CORES, PAD, width), BF16),
            VM((CORES, 128, 128), BF16),
            VM((CORES, 8, 128), F32),
            VM((128, 128), BF16),
            VM((STEPS, 128, 128), BF16),
            VM((8, 128), F32),
            VM((STEPS, 8, 128), F32),
            VM((CORES, 128, 128), BF16),
            VM((CORES, 128, 128), F32),
            VM((128, 128), F32),
            VM((128, 512), F32),
            dma((4, 4)), dma((4, 4)), dma((4, 4)), dma((4, 4)), dma((4, 8)), dma((4, 8)),
            dma((4,)), dma((4,)),
            dma((2,)), dma((2,)), dma((2,)), dma((6,)), dma((6,)), dma((8,)), dma((8,)),
            dma((4,)), dma((4,)), dma((5, 4)), dma((4, 4)), dma((5,)), dma((4,)),
            dma((4, 4)), dma((4, 4)),
            dma((2, 8)), dma((2, 8)), dma((3, 2)), dma((3, 2)), dma((4, 2)), dma((4, 2)),
            dma((8,)), dma((8,)), dma((8,)), dma((8,)), dma((8,)), dma((8,)),
            dma((8,)), dma((8,)), dma((8,)), dma((8,)),
        ],
        compiler_params=pltpu.CompilerParams(
            collective_id=1, has_side_effects=True, vmem_limit_bytes=58 << 20
        ),
        name="spread",
    )(*operands)


def state_body(inputs, gate, inflow, readout, cum, cum_t, step_t, skip, ent, out, gated, g):
    low = lax.broadcasted_iota(jnp.int32, (128, 128), 1) < 64
    causal = lax.broadcasted_iota(jnp.int32, (128, 128), 0) >= lax.broadcasted_iota(
        jnp.int32, (128, 128), 1)
    cols = slice(128 * g, 128 * g + 128)
    read = readout[:, g, :]
    rw = lax.dot_general(
        read, inflow[:, g, :], (((1,), (1,)), ((), ())), preferred_element_type=F32
    )
    square = jnp.zeros((128, 1), F32)
    for p in range(4):
        pair = 4 * g + p
        at = slice(128 * pair, 128 * pair + 128)
        both = inputs[:, at]
        parts = []
        scales = []
        for h in range(2):
            head = 2 * pair + h
            own = cum[:, head:head + 1]
            gap = jnp.where(causal, own - cum_t[head:head + 1, :], 0.0)
            mixing = jnp.where(causal, jnp.exp(gap), 0.0) * rw * step_t[head:head + 1, :]
            parts.append(
                jnp.dot(mixing.astype(BF16), both, preferred_element_type=F32)
            )
            scales.append(jnp.exp(own))
        intra = jnp.where(low, parts[0], parts[1])
        scale = jnp.where(low, scales[0], scales[1])
        inter = scale * lax.dot_general(
            read, ent[pair], (((1,), (1,)), ((), ())), preferred_element_type=F32
        )
        direct = jnp.where(
            low, skip[:, 2 * pair:2 * pair + 1], skip[:, 2 * pair + 1:2 * pair + 2]
        )
        mixed = intra + inter + direct * both.astype(F32)
        v = gate[:, at].astype(F32)
        value = mixed * (v / (1.0 + jnp.exp(-v)))
        gated[:, 128 * p:128 * p + 128] = value
        square = square + jnp.sum(value * value, axis=1, keepdims=True)
    inv = lax.rsqrt(square / 512.0 + EPSILON)
    wide = slice(512 * g, 512 * g + 512)
    out[:, wide] = gated[...] * inv


def local(
    query_heads, key_heads, value_head_rows, state_input, state_gate, state_inflow,
    state_readout, step_size, log_decay, skip_scale, state_gain, hidden_in, mlp_gain,
    router_weight, expert_ids, slot_index, gate_up, down_proj,
):
    kv_in = jnp.concatenate(
        [jnp.transpose(key_heads, (1, 0, 2)), jnp.transpose(value_head_rows, (1, 0, 2))], axis=0
    )
    heads, states, total = spread(
        kv_in, hidden_in, mlp_gain[None], router_weight.T, expert_ids.T, slot_index.T,
        jnp.transpose(gate_up[0], (1, 0, 2)), down_proj[0],
        query_heads,
        state_input, state_gate, state_inflow, state_readout,
        log_decay.T, step_size.T, skip_scale[None],
    )
    window_out = jnp.transpose(heads.reshape(8, 128, 128), (1, 0, 2))
    return window_out, (states * state_gain).astype(BF16), total.astype(BF16)


def solution(mesh):
    both = ("seq", "exp")
    placed = (
        P(both, "tp", None), P(both, "tp", None), P(both, "tp", None),
        P(both, "tp"), P(both, "tp"), P(both, "tp", None), P(both, "tp", None),
        P(both, "tp"), P(both, "tp"), P("tp"), P("tp"), P(both, None), P(), P(),
        P(both, None), P(both, None),
        P("exp", ("seq", "tp"), None, None), P("exp", ("seq", "tp"), None),
    )
    return jax.shard_map(
        local,
        mesh=mesh,
        in_specs=placed,
        out_specs=(P(both, "tp", None), P(both, "tp"), P(both, "tp")),
        check_vma=False,
    )
```
